32 devices in a mesh: group: 2 (over y), seq: 4 (over z), tensor: 4 (over x, core).
Axes of the slice: x: 2, y: 2, z: 4, core: 2. Of those that a mesh axis runs over, the one named last changes fastest.
Arguments:
- query: bfloat16 [16, 7168], P(('group', 'seq'), 'tensor'), parts along dimension 0, may hold values from -5 to 5
- key_cache: bfloat16 [32, 256, 7168], P(('group', 'seq'), None, 'tensor'), parts along dimension 0, may hold values from -5 to 5
- value_cache: bfloat16 [32, 256, 7168], P(('group', 'seq'), None, 'tensor'), parts along dimension 0, may hold values from -6 to 6
- alibi_slopes: float32 [56], P('tensor'), may hold values from 0 to 1, as said below
- block_seq: int32 [32], P(('group', 'seq')), parts along dimension 0, may hold values from 0 to 7, as said below
- block_pos: int32 [32], P(('group', 'seq')), parts along dimension 0, may hold values from 0 to 2, as said below
- lengths: int32 [16], P('group'), parts along dimension 0, may hold values from 1 to 768, as said below
- out_weight: bfloat16 [7168, 14336], P('tensor', 'seq'), may hold values from -0.5 to 0.5
Outputs:
- mixed: bfloat16 [16, 14336], P(('group', 'tensor'), 'seq'), parts along dimension 0
The draws below stay inside these ranges and needn't reach their ends.
There are 2 independent parts, one for each index of `group`. The reference program is written for one: setup_inputs(seed, part) draws one part's arguments, and reference() takes and returns one part's arrays. A program takes and returns all parts, laid end to end along the dimension named above; an argument that names none is the same for every part. Nothing has to cross between parts.
Inputs may be any that keep to these rules, and one draw needn't show every extreme that they name: `block_seq`: every sequence owns at least one block and at most 3; the blocks of sequence s have block_pos 0 to n_s - 1, each once. block_pos of a block is below the number of blocks its sequence owns. `lengths`: A sequence that owns n blocks has a length above 256 * (n - 1) and at most 256 * n. `alibi_slopes`: positive slopes.
All inputs are finite; a program needn't handle non-finite values.
Results may differ from the reference program's by a relative error of at most 0.0054.
Values may be sent and summed in bfloat16 or wider, within the bound.
A program may use at most 64 MiB of HBM per device.

```python
import math
import jax
import jax.numpy as jnp
from jax import lax

D = 14336
HEADS = 56
HEAD_DIM = 128
BLOCK = 256
SEQS = 8
BLOCKS = 16
MOST_BLOCKS = 3


def block_layout(key):
    second = jax.random.fold_in(key, 12)
    third = jax.random.fold_in(key, 13)
    fourth = jax.random.fold_in(key, 14)
    fifth = jax.random.fold_in(key, 15)
    extra = BLOCKS - SEQS
    capacity = MOST_BLOCKS - 1
    remain = extra - capacity
    relabel = jax.random.permutation(third, SEQS).astype(jnp.int32)
    longest = relabel[0]
    seq_ids = jnp.arange(SEQS, dtype=jnp.int32)
    counts = 1 + capacity * (seq_ids == longest).astype(jnp.int32)
    if remain > 0:
        order = jax.random.permutation(second, (SEQS - 1) * capacity)[:remain].astype(jnp.int32)
        target = relabel[1 + order // capacity]
        counts = counts + jnp.sum((target[:, None] == seq_ids[None, :]).astype(jnp.int32), axis=0)
    ends = jnp.cumsum(counts).astype(jnp.int32)
    starts = ends - counts
    slots = jnp.arange(BLOCKS, dtype=jnp.int32)
    seq_of = jnp.sum((ends[None, :] <= slots[:, None]).astype(jnp.int32), axis=1)
    pos_of = slots - starts[seq_of]
    placed = jax.random.permutation(fourth, BLOCKS)
    owners = jnp.zeros((BLOCKS,), jnp.int32).at[placed].set(seq_of)
    places = jnp.zeros((BLOCKS,), jnp.int32).at[placed].set(pos_of)
    tails = jax.random.randint(fifth, (SEQS,), 1, BLOCK + 1).astype(jnp.int32)
    tails = jnp.where(seq_ids == longest, BLOCK, tails)
    sizes_out = ((counts - 1) * BLOCK + tails).astype(jnp.int32)
    return (owners, places, sizes_out)


def draw_block_seq(key, part):
    return block_layout(key)[0]


def draw_block_pos(key, part):
    return block_layout(key)[1]


def draw_lengths(key, part):
    return block_layout(key)[2]


def draw_query(key, part):
    base = jnp.clip(jax.random.normal(jax.random.fold_in(key, 21), (SEQS, HEADS, HEAD_DIM), jnp.float32), -5.0, 5.0)
    return base.reshape(SEQS, HEADS * HEAD_DIM).astype(jnp.bfloat16)


def draw_key_cache(key, part):
    base = jnp.clip(jax.random.normal(jax.random.fold_in(key, 23), (BLOCKS, BLOCK, HEADS * HEAD_DIM), jnp.float32), -5.0, 5.0)
    return base.astype(jnp.bfloat16)


def draw_alibi_slopes(key, part):
    spread = jax.random.uniform(jax.random.fold_in(key, 32), (HEADS,), jnp.float32)
    strong = jax.random.randint(jax.random.fold_in(key, 31), (HEADS,), 0, 2) == 1
    slow = jnp.exp(jnp.log(1.0 / 8192.0) + spread * jnp.log(8.0))
    fast = jnp.exp(jnp.log(1.0 / 64.0) + spread * jnp.log(8.0))
    return jnp.where(strong, fast, slow).astype(jnp.float32)


def steps_of(rng, shape, shards, least, high):
    factor_of, own = 1.0, jax.random.fold_in(rng, 6)
    for axis_at, parts in shards:
        steps = jnp.exp(jax.random.uniform(jax.random.fold_in(own, axis_at), (parts,), jnp.float32, least / len(shards), high / len(shards)))
        factor_of = factor_of * jnp.repeat(steps, shape[axis_at] // parts).reshape([-1 if axis == axis_at else 1 for axis in range(len(shape))])
    return factor_of


def scatter_about(rng, extent, deviation, bound, split=(), kind=jnp.bfloat16):
    array = jax.random.normal(rng, extent, jnp.float32) * deviation
    if len(split) > 0:
        array = steps_of(rng, extent, split, -0.22, 0.18) * array
    return jnp.clip(array, min=-bound, max=bound).astype(kind)


def setup_inputs(seed: int = 0, part: int = 0) -> dict:
    streams_of = jax.random.split(jax.random.key(seed), 9)
    part_keys = jax.random.split(jax.random.fold_in(streams_of[8], part), 9)
    return {
        "query": draw_query(jax.random.fold_in(jax.random.fold_in(streams_of[8], part), 71), part),
        "key_cache": draw_key_cache(jax.random.fold_in(jax.random.fold_in(streams_of[8], part), 71), part),
        "value_cache": scatter_about(part_keys[2], (BLOCKS, BLOCK, HEADS * HEAD_DIM), 1.0, 6.0, ((0, 4), (2, 4))),
        "alibi_slopes": draw_alibi_slopes(jax.random.fold_in(streams_of[8], 71), part),
        "block_seq": draw_block_seq(jax.random.fold_in(jax.random.fold_in(streams_of[8], part), 71), part),
        "block_pos": draw_block_pos(jax.random.fold_in(jax.random.fold_in(streams_of[8], part), 71), part),
        "lengths": draw_lengths(jax.random.fold_in(jax.random.fold_in(streams_of[8], part), 71), part),
        "out_weight": scatter_about(streams_of[7], (HEADS * HEAD_DIM, D), HEAD_DIM ** -0.5, 0.5, ((0, 4), (1, 4))),
    }


def reference(query, key_cache, value_cache, alibi_slopes, block_seq, block_pos, lengths, out_weight):
    scale = 1.0 / math.sqrt(HEAD_DIM)
    offsets = jnp.arange(BLOCK, dtype=jnp.int32)

    def one_block(index):
        owner = block_seq[index]
        length = lengths[owner]
        placed = block_pos[index] * BLOCK + offsets
        live = placed < length
        qrow = query[owner].astype(jnp.float32).reshape(HEADS, HEAD_DIM)
        keys = key_cache[index].astype(jnp.float32).reshape(BLOCK, HEADS, HEAD_DIM)
        values = value_cache[index].astype(jnp.float32).reshape(BLOCK, HEADS, HEAD_DIM)
        scores = jnp.einsum('thd,hd->ht', keys, qrow) * scale
        distance = (length - 1 - placed).astype(jnp.float32)
        scores = scores - alibi_slopes[:, None] * distance[None, :]
        scores = jnp.where(live[None, :], scores, -1e+30)
        top = lax.optimization_barrier(jnp.max(scores, axis=1))
        weights = jnp.where(live[None, :], jnp.exp(scores - top[:, None]), 0.0)
        total = lax.optimization_barrier(jnp.sum(weights, axis=1))
        rounded = lax.optimization_barrier(weights.astype(jnp.bfloat16)).astype(jnp.float32)
        summed = jnp.einsum('ht,thd->hd', rounded, values)
        return (top, total, summed)
    tops, totals, sums = lax.map(one_block, jnp.arange(BLOCKS, dtype=jnp.int32))
    seq_ids = jnp.arange(SEQS, dtype=jnp.int32)
    owned = block_seq[None, :] == seq_ids[:, None]
    seq_max = lax.optimization_barrier(jnp.max(jnp.where(owned[:, :, None], tops[None], -1e+30), axis=1))
    factor = jnp.where(owned[:, :, None], jnp.exp(tops[None] - seq_max[:, None, :]), 0.0)
    seq_sum = lax.optimization_barrier(jnp.sum(factor * totals[None], axis=1))
    seq_acc = jnp.einsum('sbh,bhd->shd', factor, sums, precision=lax.Precision.HIGHEST)
    attention = (seq_acc / seq_sum[:, :, None]).reshape(SEQS, HEADS * HEAD_DIM).astype(jnp.bfloat16)
    return jnp.dot(attention, out_weight, preferred_element_type=jnp.float32).astype(jnp.bfloat16)
```

```python
import functools
import math

import jax
import jax.numpy as jnp
from jax import lax
from jax.experimental import pallas as pl
from jax.experimental.pallas import tpu as pltpu
from jax.sharding import PartitionSpec as P

LANES = 128
OWNER_LANE = LANES - 1


def kernel(
    seq_size, tensor_size, groups, chunks,
    block_seq_in, block_pos_in, lengths_in, slopes_in, query, keys, values, weight,
    out,
    block_seq, block_pos, lengths, slopes,
    q_all, k_buf, v_buf, w_buf, stats, accs, held, part, landed,
    small_sem, q_sem, k_sem, v_sem, w_sem,
    q_send, q_recv, s_send, s_recv, a_send, a_recv, p_send, p_recv,
):
    me = lax.axis_index("seq")
    my_rows = lax.axis_index("tensor")
    blocks, block_len, features = k_buf.shape
    heads = slopes.shape[0]
    size = features // heads
    seqs = lengths.shape[0]
    query_rows = q_all.shape[1]
    rows, width = part.shape[2:]
    scale = 1.0 / math.sqrt(size)

    barrier = pltpu.get_barrier_semaphore()
    for k in range(1, seq_size):
        pl.semaphore_signal(barrier, inc=1, device_id={"seq": lax.rem(me + k, seq_size)})
    for k in range(1, tensor_size):
        pl.semaphore_signal(
            barrier, inc=1, device_id={"tensor": lax.rem(my_rows + k, tensor_size)}
        )
    q_copy = pltpu.make_async_copy(query, q_all.at[me], q_sem)
    q_copy.start()
    small_copies = [
        pltpu.make_async_copy(source, target, small_sem.at[i])
        for i, (source, target) in enumerate(
            [
                (block_seq_in, block_seq),
                (block_pos_in, block_pos),
                (lengths_in, lengths),
                (slopes_in, slopes),
            ]
        )
    ]
    for copy in small_copies:
        copy.start()
    cache_copies = [
        pltpu.make_async_copy(cache.at[b], buffer.at[b], sem)
        for cache, buffer, sem in ((keys, k_buf, k_sem), (values, v_buf, v_sem))
        for b in range(blocks)
    ]
    spans = [(first * size, last * size) for first, last in groups]
    w_copies = [
        pltpu.make_async_copy(
            weight.at[pl.ds(low, high - low)], w_buf.at[pl.ds(low, high - low)], w_sem.at[g]
        )
        for g, (low, high) in enumerate(spans)
    ]

    q_copy.wait()
    for copy in cache_copies:
        copy.start()
    pl.semaphore_wait(barrier, seq_size + tensor_size - 2)

    stride = jnp.where(me < seq_size // 2, seq_size - 1, 1)

    def drain(ref, sem):
        pltpu.make_async_copy(ref, ref, sem).wait()

    def to_seq(buffer, send, recv):
        copies = [
            pltpu.make_async_remote_copy(
                src_ref=buffer.at[me],
                dst_ref=buffer.at[me],
                send_sem=send,
                recv_sem=recv,
                device_id={"seq": lax.rem(me + stride * k, seq_size)},
            )
            for k in range(1, seq_size)
        ]
        for copy in copies:
            copy.start()

    to_seq(q_all, q_send, q_recv)

    for copy in small_copies:
        copy.wait()
    offsets = lax.broadcasted_iota(jnp.int32, (1, block_len), 1)
    stat_lane = lax.broadcasted_iota(jnp.int32, (1, LANES), 1)

    others = pl.ds(0, seq_size - 1)
    drain(k_buf, k_sem)
    drain(v_buf, v_sem)
    for copy in w_copies:
        copy.start()
    drain(q_all.at[others], q_recv)

    q_rows = []
    for b in range(blocks):
        owner = block_seq[b]
        near = q_all[lax.div(owner, query_rows)].astype(jnp.float32)
        which = lax.rem(owner, query_rows)
        q_row = near[:1]
        for r in range(1, query_rows):
            q_row = jnp.where(which == r, near[r : r + 1], q_row)
        q_rows.append(q_row)

    for g, (first, last) in enumerate(groups):
        low, high = spans[g]
        padded = -(-(last - first) // 16) * 16
        lane = lax.broadcasted_iota(jnp.int32, (padded, high - low), 1)
        row = lax.broadcasted_iota(jnp.int32, (padded, high - low), 0)
        of_head = (lane >= row * size) & (lane < row * size + size)
        head_row = lax.broadcasted_iota(jnp.int32, (padded, LANES), 0)
        head_lane = lax.broadcasted_iota(jnp.int32, (padded, LANES), 1)
        slope = jnp.zeros((padded, LANES), jnp.float32)
        for h in range(first, last):
            slope = jnp.where(head_row == h - first, slopes[h], slope)
        slope = slope[:, :1]
        weights, inverse, stat_rows = [], [], []
        for b in range(blocks):
            owner = block_seq[b]
            length = lengths[owner]
            spread = jnp.where(of_head, q_rows[b][:, low:high], 0.0).astype(jnp.bfloat16)
            scores = lax.dot_general(
                spread,
                k_buf[b, :, low:high],
                (((1,), (1,)), ((), ())),
                preferred_element_type=jnp.float32,
            )
            placed = block_pos[b] * block_len + offsets
            live = placed < length
            distance = (length - 1 - placed).astype(jnp.float32)
            scores = jnp.where(live, scores * scale - slope * distance, -1e30)
            top = jnp.max(scores, axis=1, keepdims=True)
            weight_b = jnp.where(live, jnp.exp(scores - top), 0.0)
            total = jnp.sum(weight_b, axis=1, keepdims=True)
            weights.append(weight_b.astype(jnp.bfloat16))
            inverse.append(1.0 / total)
            stat = jnp.sum(
                jnp.where(head_row == head_lane, top + jnp.log(total), 0.0), axis=0, keepdims=True
            )
            stat_rows.append(jnp.where(stat_lane == OWNER_LANE, owner.astype(jnp.float32), stat))
        stats[g][me] = jnp.concatenate(stat_rows, axis=0)
        to_seq(stats[g], s_send.at[g], s_recv.at[g])
        acc_rows = []
        for b in range(blocks):
            summed = jnp.dot(
                weights[b], v_buf[b, :, low:high], preferred_element_type=jnp.float32
            )
            summed = summed * inverse[b]
            acc_rows.append(jnp.sum(jnp.where(of_head, summed, 0.0), axis=0, keepdims=True))
        accs[g][me] = jnp.concatenate(acc_rows, axis=0).astype(jnp.bfloat16)
        to_seq(accs[g], a_send.at[g], a_recv.at[g])

    def attention_of(g):
        drain(stats[g].at[others], s_recv.at[g])
        stat = stats[g][...]
        owners = stat[:, :, OWNER_LANE:]
        best = jnp.zeros_like(stat)
        masks = [owners == float(s) for s in range(seqs)]
        for s in range(seqs):
            top = jnp.max(jnp.where(masks[s], stat, -1e30), axis=(0, 1), keepdims=True)
            best = jnp.where(masks[s], top, best)
        grown = jnp.exp(stat - best)
        whole = jnp.ones_like(stat)
        for s in range(seqs):
            total = jnp.sum(jnp.where(masks[s], grown, 0.0), axis=(0, 1), keepdims=True)
            whole = jnp.where(masks[s], total, whole)
        factor = grown / whole
        seq_lane = lax.broadcasted_iota(jnp.int32, (blocks, LANES), 1).astype(jnp.float32)
        owned = jnp.concatenate(
            [jnp.where(owners[j] == seq_lane, 1.0, 0.0) for j in range(seq_size)], axis=0
        )
        owned = owned.T[:seqs].astype(jnp.bfloat16)
        first, last = groups[g]
        spread = [
            jnp.concatenate(
                [
                    jnp.broadcast_to(factor[j][:, h : h + 1], (blocks, size))
                    for h in range(last - first)
                ],
                axis=1,
            )
            for j in range(seq_size)
        ]
        drain(accs[g].at[others], a_recv.at[g])
        w_copies[g].wait()
        scaled = jnp.concatenate(
            [accs[g][j].astype(jnp.float32) * spread[j] for j in range(seq_size)], axis=0
        )
        upper = scaled.astype(jnp.bfloat16)
        lower = (scaled - upper.astype(jnp.float32)).astype(jnp.bfloat16)
        attention = jnp.dot(owned, upper, preferred_element_type=jnp.float32) + jnp.dot(
            owned, lower, preferred_element_type=jnp.float32
        )
        return attention.astype(jnp.bfloat16)

    for g, (low, high) in enumerate(spans[:-1]):
        attention = attention_of(g)
        product = jnp.dot(attention, w_buf[low:high], preferred_element_type=jnp.float32)
        held[...] = product if g == 0 else held[...] + product
    attention = attention_of(len(groups) - 1)
    low, high = spans[-1]

    def product_of(c):
        columns = slice(c * width, (c + 1) * width)
        product = jnp.dot(attention, w_buf[low:high, columns], preferred_element_type=jnp.float32)
        return product + held[:, columns]

    later = product_of(0)
    for c in range(chunks):
        product = later
        if c + 1 < chunks:
            later = product_of(c + 1)
        for r in range(tensor_size):
            part[r, c] = product[r * rows : (r + 1) * rows].astype(part.dtype)
        for k in range(1, tensor_size):
            peer = lax.rem(my_rows + k, tensor_size)
            pltpu.make_async_remote_copy(
                src_ref=part.at[peer, c],
                dst_ref=landed.at[k - 1, c],
                send_sem=p_send,
                recv_sem=p_recv,
                device_id={"tensor": peer},
            ).start()
    drain(landed, p_recv)
    for c in range(chunks):
        total = part[my_rows, c].astype(jnp.float32)
        for k in range(1, tensor_size):
            total = total + landed[k - 1, c].astype(jnp.float32)
        out[:, c * width : (c + 1) * width] = total.astype(out.dtype)
    drain(q_all.at[others], q_send)
    for g in range(len(groups)):
        drain(stats[g].at[others], s_send.at[g])
        drain(accs[g].at[others], a_send.at[g])
    drain(landed, p_send)


def local(seq_size, tensor_size, query, key_cache, value_cache, slopes, block_seq, block_pos, lengths, weight):
    heads = slopes.shape[0]
    blocks, block_len, features = key_cache.shape
    size = features // heads
    columns = weight.shape[1]
    chunks = max([c for c in range(1, 9) if columns % (c * 256) == 0], default=1)
    width = columns // chunks
    rows = lengths.shape[0] // tensor_size
    middle = min(heads, -(-heads // 4) * 2)
    groups = [(low, high) for low, high in ((0, middle), (middle, heads)) if high > low]
    smalls = (block_seq, block_pos, lengths, slopes)
    dma = pltpu.SemaphoreType.DMA
    return pl.pallas_call(
        functools.partial(kernel, seq_size, tensor_size, groups, chunks),
        out_shape=pltpu.VMEM((rows, columns), jnp.bfloat16),
        in_specs=[pl.BlockSpec(memory_space=pltpu.HBM)] * 8,
        out_specs=pl.BlockSpec(memory_space=pltpu.VMEM),
        scratch_shapes=[pltpu.SMEM(a.shape, a.dtype) for a in smalls]
        + [
            pltpu.VMEM((seq_size,) + query.shape, query.dtype),
            pltpu.VMEM(key_cache.shape, key_cache.dtype),
            pltpu.VMEM(value_cache.shape, value_cache.dtype),
            pltpu.VMEM(weight.shape, weight.dtype),
            [pltpu.VMEM((seq_size, blocks, LANES), jnp.float32) for _ in groups],
            [
                pltpu.VMEM((seq_size, blocks, (high - low) * size), jnp.bfloat16)
                for low, high in groups
            ],
            pltpu.VMEM((lengths.shape[0], columns), jnp.float32),
            pltpu.VMEM((tensor_size, chunks, rows, width), jnp.bfloat16),
            pltpu.VMEM((tensor_size - 1, chunks, rows, width), jnp.bfloat16),
            dma((4,)),
            dma,
            dma,
            dma,
            dma((len(groups),)),
        ]
        + [dma] * 2
        + [dma((len(groups),))] * 4
        + [dma] * 2,
        compiler_params=pltpu.CompilerParams(
            collective_id=0, has_side_effects=True, vmem_limit_bytes=48 * 1024 * 1024
        ),
    )(
        *[
            pltpu.with_memory_space_constraint(a, pltpu.HBM)
            for a in smalls + (query, key_cache, value_cache, weight)
        ]
    )


def solution(mesh):
    placed = (
        P(("group", "seq"), "tensor"),
        P(("group", "seq"), None, "tensor"),
        P(("group", "seq"), None, "tensor"),
        P("tensor"),
        P(("group", "seq")),
        P(("group", "seq")),
        P("group"),
        P("tensor", "seq"),
    )
    return jax.shard_map(
        functools.partial(local, mesh.shape["seq"], mesh.shape["tensor"]),
        mesh=mesh,
        in_specs=placed,
        out_specs=P(("group", "tensor"), "seq"),
        check_vma=False,
    )
```

```python
import functools
import math

import jax
import jax.numpy as jnp
from jax import lax
from jax.experimental import pallas as pl
from jax.experimental.pallas import tpu as pltpu
from jax.sharding import PartitionSpec as P

LANES = 128
OWNER_LANE = LANES - 1


def kernel(
    seq_size, tensor_size, groups, chunks,
    block_seq_in, block_pos_in, lengths_in, slopes_in, query, keys, values, weight,
    out,
    block_seq, block_pos, lengths, slopes,
    q_all, k_buf, kt_buf, v_buf, w_buf, stats, accs, held, part, landed,
    small_sem, q_sem, k_sem, v_sem, w_sem,
    q_send, q_recv, s_send, s_recv, a_send, a_recv, p_send, p_recv,
):
    me = lax.axis_index("seq")
    my_rows = lax.axis_index("tensor")
    blocks, block_len, features = k_buf.shape
    heads = slopes.shape[0]
    size = features // heads
    seqs = lengths.shape[0]
    query_rows = q_all.shape[1]
    rows, width = part.shape[2:]
    scale = 1.0 / math.sqrt(size)

    barrier = pltpu.get_barrier_semaphore()
    for k in range(1, seq_size):
        pl.semaphore_signal(barrier, inc=1, device_id={"seq": lax.rem(me + k, seq_size)})
    for k in range(1, tensor_size):
        pl.semaphore_signal(
            barrier, inc=1, device_id={"tensor": lax.rem(my_rows + k, tensor_size)}
        )
    q_copy = pltpu.make_async_copy(query, q_all.at[me], q_sem)
    q_copy.start()
    small_copies = [
        pltpu.make_async_copy(source, target, small_sem.at[i])
        for i, (source, target) in enumerate(
            [
                (block_seq_in, block_seq),
                (block_pos_in, block_pos),
                (lengths_in, lengths),
                (slopes_in, slopes),
            ]
        )
    ]
    for copy in small_copies:
        copy.start()
    cache_copies = [
        pltpu.make_async_copy(keys.at[b], k_buf.at[b], k_sem.at[b]) for b in range(blocks)
    ] + [pltpu.make_async_copy(values.at[b], v_buf.at[b], v_sem) for b in range(blocks)]
    spans = [(first * size, last * size) for first, last in groups]
    w_copies = [
        pltpu.make_async_copy(
            weight.at[pl.ds(low, high - low)], w_buf.at[pl.ds(low, high - low)], w_sem.at[g]
        )
        for g, (low, high) in enumerate(spans)
    ]

    q_copy.wait()
    for copy in cache_copies:
        copy.start()
    pl.semaphore_wait(barrier, seq_size + tensor_size - 2)

    stride = jnp.where(me < seq_size // 2, seq_size - 1, 1)

    def drain(ref, sem):
        pltpu.make_async_copy(ref, ref, sem).wait()

    def to_seq(buffer, send, recv):
        copies = [
            pltpu.make_async_remote_copy(
                src_ref=buffer.at[me],
                dst_ref=buffer.at[me],
                send_sem=send,
                recv_sem=recv,
                device_id={"seq": lax.rem(me + stride * k, seq_size)},
            )
            for k in range(1, seq_size)
        ]
        for copy in copies:
            copy.start()

    to_seq(q_all, q_send, q_recv)

    for copy in small_copies:
        copy.wait()
    offsets = lax.broadcasted_iota(jnp.int32, (1, block_len), 1)
    stat_lane = lax.broadcasted_iota(jnp.int32, (1, LANES), 1)

    others = pl.ds(0, seq_size - 1)
    for b in range(blocks):
        cache_copies[b].wait()
        for low in range(0, features, size):
            kt_buf[b, low : low + size, :] = k_buf[b, :, low : low + size].T
    drain(v_buf, v_sem)
    for copy in w_copies:
        copy.start()
    drain(q_all.at[others], q_recv)

    owners = [block_seq[b] for b in range(blocks)]
    q_rows, live, distance = [], [], []
    for b in range(blocks):
        near = q_all[lax.div(owners[b], query_rows)].astype(jnp.float32)
        which = lax.rem(owners[b], query_rows)
        q_row = near[:1]
        for r in range(1, query_rows):
            q_row = jnp.where(which == r, near[r : r + 1], q_row)
        q_rows.append(q_row)
        length = lengths[owners[b]]
        placed = block_pos[b] * block_len + offsets
        live.append(placed < length)
        distance.append((length - 1 - placed).astype(jnp.float32))

    def masks_of(g):
        low, high = spans[g]
        padded = -(-(high - low) // (16 * size)) * 16
        lane = lax.broadcasted_iota(jnp.int32, (padded, high - low), 1)
        row = lax.broadcasted_iota(jnp.int32, (padded, high - low), 0)
        head_row = lax.broadcasted_iota(jnp.int32, (padded, LANES), 0)
        head_lane = lax.broadcasted_iota(jnp.int32, (padded, LANES), 1)
        first, last = groups[g]
        slope = jnp.zeros((padded, LANES), jnp.float32)
        for h in range(first, last):
            slope = jnp.where(head_row == h - first, slopes[h], slope)
        return (lane >= row * size) & (lane < row * size + size), head_row == head_lane, slope[:, :1]

    masks = [masks_of(g) for g in range(len(groups))]

    def scores_of(g):
        low, high = spans[g]
        return [
            jnp.dot(
                jnp.where(masks[g][0], q_rows[b][:, low:high], 0.0).astype(jnp.bfloat16),
                kt_buf[b, low:high, :],
                preferred_element_type=jnp.float32,
            )
            for b in range(blocks)
        ]

    def values_of(g, scores):
        low, high = spans[g]
        of_head, diagonal, slope = masks[g]
        summed, inverse, stat_rows = [], [], []
        for b in range(blocks):
            score = jnp.where(live[b], scores[b] * scale - slope * distance[b], -1e30)
            top = jnp.max(score, axis=1, keepdims=True)
            weight_b = jnp.where(live[b], jnp.exp(score - top), 0.0)
            summed.append(
                jnp.dot(
                    weight_b.astype(jnp.bfloat16),
                    v_buf[b, :, low:high],
                    preferred_element_type=jnp.float32,
                )
            )
            total = jnp.sum(weight_b, axis=1, keepdims=True)
            inverse.append(1.0 / total)
            stat = jnp.sum(
                jnp.where(diagonal, top + jnp.log(total), 0.0), axis=0, keepdims=True
            )
            stat_rows.append(
                jnp.where(stat_lane == OWNER_LANE, owners[b].astype(jnp.float32), stat)
            )
        stats[g][me] = jnp.concatenate(stat_rows, axis=0)
        to_seq(stats[g], s_send.at[g], s_recv.at[g])
        acc_rows = [
            jnp.sum(jnp.where(of_head, summed[b] * inverse[b], 0.0), axis=0, keepdims=True)
            for b in range(blocks)
        ]
        accs[g][me] = jnp.concatenate(acc_rows, axis=0).astype(jnp.bfloat16)
        to_seq(accs[g], a_send.at[g], a_recv.at[g])

    scores = [scores_of(g) for g in range(min(2, len(groups)))]
    for g in range(len(groups)):
        values_of(g, scores[g])
        if g + 2 < len(groups):
            scores.append(scores_of(g + 2))

    def joined(ref):
        return jnp.concatenate([ref[j].astype(jnp.float32) for j in range(seq_size)], axis=0)

    def factors_of(g):
        stat = joined(stats[g])
        owner = stat[:, OWNER_LANE:]
        best, whole = jnp.zeros_like(stat), jnp.ones_like(stat)
        owned = [owner == float(s) for s in range(seqs)]
        for s in range(seqs):
            top = jnp.max(jnp.where(owned[s], stat, -1e30), axis=0, keepdims=True)
            best = jnp.where(owned[s], top, best)
        grown = jnp.exp(stat - best)
        for s in range(seqs):
            total = jnp.sum(jnp.where(owned[s], grown, 0.0), axis=0, keepdims=True)
            whole = jnp.where(owned[s], total, whole)
        factor = grown / whole
        first, last = groups[g]
        spread = jnp.concatenate(
            [jnp.broadcast_to(factor[:, h : h + 1], (factor.shape[0], size)) for h in range(last - first)],
            axis=1,
        )
        return spread, owner

    def attention_of(g):
        spread, owner = factors_of(g)
        scaled = joined(accs[g]) * spread
        seq_row = lax.broadcasted_iota(jnp.int32, (seqs, LANES), 0).astype(jnp.float32)
        if seqs <= 16:
            parts = []
            for low in range(0, scaled.shape[1], LANES):
                part_sum = jnp.zeros((seqs, LANES), jnp.float32)
                for i in range(scaled.shape[0]):
                    part_sum = part_sum + jnp.where(
                        owner[i : i + 1] == seq_row, scaled[i : i + 1, low : low + LANES], 0.0
                    )
                parts.append(part_sum)
            attention = jnp.concatenate(parts, axis=1)
        else:
            seq_lane = lax.broadcasted_iota(jnp.int32, (scaled.shape[0], LANES), 1)
            owned = jnp.where(owner == seq_lane.astype(jnp.float32), 1.0, 0.0)
            owned = owned.T[:seqs].astype(jnp.bfloat16)
            upper = scaled.astype(jnp.bfloat16)
            lower = (scaled - upper.astype(jnp.float32)).astype(jnp.bfloat16)
            attention = jnp.dot(owned, upper, preferred_element_type=jnp.float32) + jnp.dot(
                owned, lower, preferred_element_type=jnp.float32
            )
        return attention.astype(jnp.bfloat16)

    def project(g, attention, left, right):
        if left == right:
            return
        low, high = spans[g]
        product = jnp.dot(
            attention, w_buf[low:high, left:right], preferred_element_type=jnp.float32
        )
        held[:, left:right] = product if g == 0 else held[:, left:right] + product

    half = chunks // 2 * width
    columns_of = held.shape[1]
    attention = None
    for g, (low, high) in enumerate(spans):
        drain(stats[g].at[others], s_recv.at[g])
        drain(accs[g].at[others], a_recv.at[g])
        w_copies[g].wait()
        if g > 0:
            project(g - 1, attention, half, columns_of)
        attention = attention_of(g)
        if g + 1 < len(groups):
            project(g, attention, 0, half)

    def product_of(c):
        columns = slice(c * width, (c + 1) * width)
        product = jnp.dot(attention, w_buf[low:high, columns], preferred_element_type=jnp.float32)
        return product + held[:, columns]

    later = product_of(0)
    for c in range(chunks):
        product = later
        if c + 1 < chunks:
            later = product_of(c + 1)
        for r in range(tensor_size):
            part[r, c] = product[r * rows : (r + 1) * rows].astype(part.dtype)
        for k in range(1, tensor_size):
            peer = lax.rem(my_rows + k, tensor_size)
            pltpu.make_async_remote_copy(
                src_ref=part.at[peer, c],
                dst_ref=landed.at[k - 1, c],
                send_sem=p_send,
                recv_sem=p_recv,
                device_id={"tensor": peer},
            ).start()
    drain(landed, p_recv)
    for c in range(chunks):
        total = part[my_rows, c].astype(jnp.float32)
        for k in range(1, tensor_size):
            total = total + landed[k - 1, c].astype(jnp.float32)
        out[:, c * width : (c + 1) * width] = total.astype(out.dtype)
    drain(q_all.at[others], q_send)
    for g in range(len(groups)):
        drain(stats[g].at[others], s_send.at[g])
        drain(accs[g].at[others], a_send.at[g])
    drain(landed, p_send)


def local(seq_size, tensor_size, query, key_cache, value_cache, slopes, block_seq, block_pos, lengths, weight):
    heads = slopes.shape[0]
    blocks, block_len, features = key_cache.shape
    size = features // heads
    columns = weight.shape[1]
    chunks = max([c for c in range(1, 9) if columns % (c * 256) == 0], default=1)
    width = columns // chunks
    rows = lengths.shape[0] // tensor_size
    outer = min(heads, -(-heads // 8) * 2)
    bounds = (0, outer, max(outer, heads - outer), heads)
    groups = [(low, high) for low, high in zip(bounds, bounds[1:]) if high > low]
    smalls = (block_seq, block_pos, lengths, slopes)
    dma = pltpu.SemaphoreType.DMA
    return pl.pallas_call(
        functools.partial(kernel, seq_size, tensor_size, groups, chunks),
        out_shape=pltpu.VMEM((rows, columns), jnp.bfloat16),
        in_specs=[pl.BlockSpec(memory_space=pltpu.HBM)] * 8,
        out_specs=pl.BlockSpec(memory_space=pltpu.VMEM),
        scratch_shapes=[pltpu.SMEM(a.shape, a.dtype) for a in smalls]
        + [
            pltpu.VMEM((seq_size,) + query.shape, query.dtype),
            pltpu.VMEM(key_cache.shape, key_cache.dtype),
            pltpu.VMEM((blocks, features, block_len), key_cache.dtype),
            pltpu.VMEM(value_cache.shape, value_cache.dtype),
            pltpu.VMEM(weight.shape, weight.dtype),
            [pltpu.VMEM((seq_size, blocks, LANES), jnp.float32) for _ in groups],
            [
                pltpu.VMEM((seq_size, blocks, (high - low) * size), jnp.bfloat16)
                for low, high in groups
            ],
            pltpu.VMEM((lengths.shape[0], columns), jnp.float32),
            pltpu.VMEM((tensor_size, chunks, rows, width), jnp.bfloat16),
            pltpu.VMEM((tensor_size - 1, chunks, rows, width), jnp.bfloat16),
            dma((4,)),
            dma,
            dma((blocks,)),
            dma,
            dma((len(groups),)),
        ]
        + [dma] * 2
        + [dma((len(groups),))] * 4
        + [dma] * 2,
        compiler_params=pltpu.CompilerParams(
            collective_id=0, has_side_effects=True, vmem_limit_bytes=48 * 1024 * 1024
        ),
    )(
        *[
            pltpu.with_memory_space_constraint(a, pltpu.HBM)
            for a in smalls + (query, key_cache, value_cache, weight)
        ]
    )


def solution(mesh):
    placed = (
        P(("group", "seq"), "tensor"),
        P(("group", "seq"), None, "tensor"),
        P(("group", "seq"), None, "tensor"),
        P("tensor"),
        P(("group", "seq")),
        P(("group", "seq")),
        P("group"),
        P("tensor", "seq"),
    )
    return jax.shard_map(
        functools.partial(local, mesh.shape["seq"], mesh.shape["tensor"]),
        mesh=mesh,
        in_specs=placed,
        out_specs=P(("group", "tensor"), "seq"),
        check_vma=False,
    )
```

```python
import functools
import math

import jax
import jax.numpy as jnp
from jax import lax
from jax.experimental import pallas as pl
from jax.experimental.pallas import tpu as pltpu
from jax.sharding import PartitionSpec as P

LANES = 128
OWNER_LANE = LANES - 1


def kernel(
    seq_size, tensor_size, groups, chunks,
    block_seq_in, block_pos_in, lengths_in, slopes_in, query, keys, values, weight,
    out,
    block_seq, block_pos, lengths, slopes,
    q_all, q_pair, k_buf, kt_buf, v_buf, w_buf, stats, accs, held, part, landed,
    small_sem, q_sem, k_sem, v_sem, w_sem,
    q_send, q_recv, pair_send, pair_recv, s_send, s_recv, a_send, a_recv, p_send, p_recv,
):
    me = lax.axis_index("seq")
    my_rows = lax.axis_index("tensor")
    blocks, block_len, features = k_buf.shape
    heads = slopes.shape[0]
    size = features // heads
    seqs = lengths.shape[0]
    query_rows = q_all.shape[1]
    rows, width = part.shape[2:]
    scale = 1.0 / math.sqrt(size)

    barrier = pltpu.get_barrier_semaphore()
    paired = tensor_size % 2 == 0
    relay = lax.rem(my_rows, 2) == 1 if paired else my_rows >= 0
    partner = my_rows + 1 - 2 * lax.rem(my_rows, 2)
    for k in range(1, seq_size):

        @pl.when(relay | (me + k < seq_size))
        def _():
            pl.semaphore_signal(barrier, inc=1, device_id={"seq": lax.rem(me + k, seq_size)})

    for k in range(1, tensor_size):
        pl.semaphore_signal(
            barrier, inc=1, device_id={"tensor": lax.rem(my_rows + k, tensor_size)}
        )
    q_copy = pltpu.make_async_copy(query, q_all.at[me], q_sem)
    q_copy.start()
    small_copies = [
        pltpu.make_async_copy(source, target, small_sem.at[i])
        for i, (source, target) in enumerate(
            [
                (block_seq_in, block_seq),
                (block_pos_in, block_pos),
                (lengths_in, lengths),
                (slopes_in, slopes),
            ]
        )
    ]
    for copy in small_copies:
        copy.start()
    cache_copies = [
        pltpu.make_async_copy(keys.at[b], k_buf.at[b], k_sem.at[b]) for b in range(blocks)
    ] + [pltpu.make_async_copy(values.at[b], v_buf.at[b], v_sem) for b in range(blocks)]
    spans = [(first * size, last * size) for first, last in groups]
    w_copies = [
        pltpu.make_async_copy(
            weight.at[pl.ds(low, high - low)], w_buf.at[pl.ds(low, high - low)], w_sem.at[g]
        )
        for g, (low, high) in enumerate(spans)
    ]

    q_copy.wait()
    for copy in cache_copies:
        copy.start()
    pl.semaphore_wait(barrier, jnp.where(relay, seq_size - 1, me) + tensor_size - 1)

    stride = jnp.where(me < seq_size // 2, seq_size - 1, 1)

    def drain(ref, sem):
        pltpu.make_async_copy(ref, ref, sem).wait()

    def to_seq(buffer, send, recv):
        copies = [
            pltpu.make_async_remote_copy(
                src_ref=buffer.at[me],
                dst_ref=buffer.at[me],
                send_sem=send,
                recv_sem=recv,
                device_id={"seq": lax.rem(me + stride * k, seq_size)},
            )
            for k in range(1, seq_size)
        ]
        for copy in copies:
            copy.start()

    def pair_copy(source, target, recv, where):
        return pltpu.make_async_remote_copy(
            src_ref=source, dst_ref=target, send_sem=pair_send, recv_sem=recv, device_id=where
        )

    if paired:

        @pl.when(jnp.logical_not(relay) & (me < seq_size - 1))
        def _():
            pair_copy(
                q_all.at[me], q_pair.at[me], pair_recv.at[me], {"tensor": partner}
            ).start()

        @pl.when(relay & (me < seq_size - 1))
        def _():
            pltpu.make_async_copy(q_pair.at[me], q_pair.at[me], pair_recv.at[me]).wait()
            for k in range(seq_size - 1, 0, -1):

                @pl.when(me + k < seq_size)
                def _():
                    pair_copy(
                        q_pair.at[me], q_pair.at[me], pair_recv.at[me], {"seq": lax.rem(me + k, seq_size)}
                    ).start()

    q_copies = []
    for k in range(1, seq_size):
        peer = lax.rem(me + stride * k, seq_size)
        copy = pltpu.make_async_remote_copy(
            src_ref=q_all.at[me],
            dst_ref=q_all.at[me],
            send_sem=q_send.at[k - 1],
            recv_sem=q_recv,
            device_id={"seq": peer},
        )
        q_copies.append((relay | (peer < me), copy))
        pl.when(q_copies[-1][0])(copy.start)

    for copy in small_copies:
        copy.wait()
    offsets = lax.broadcasted_iota(jnp.int32, (1, block_len), 1)
    stat_lane = lax.broadcasted_iota(jnp.int32, (1, LANES), 1)

    others = pl.ds(0, seq_size - 1)
    for b in range(blocks):
        cache_copies[b].wait()
        for low in range(0, features, size):
            kt_buf[b, low : low + size, :] = k_buf[b, :, low : low + size].T
    drain(v_buf, v_sem)
    for copy in w_copies:
        copy.start()
    if paired:
        for k in range(1, seq_size):

            @pl.when(relay & (me >= k))
            def _():
                lower = lax.rem(me + seq_size - k, seq_size)
                pltpu.make_async_copy(q_pair.at[lower], q_pair.at[lower], pair_recv.at[lower]).wait()
                pair_copy(q_pair.at[lower], q_all.at[lower], q_recv, {"tensor": partner}).start()

    drain(q_all.at[others], q_recv)

    owners = [block_seq[b] for b in range(blocks)]
    q_rows, live, distance = [], [], []
    for b in range(blocks):
        near = q_all[lax.div(owners[b], query_rows)].astype(jnp.float32)
        which = lax.rem(owners[b], query_rows)
        q_row = near[:1]
        for r in range(1, query_rows):
            q_row = jnp.where(which == r, near[r : r + 1], q_row)
        q_rows.append(q_row)
        length = lengths[owners[b]]
        placed = block_pos[b] * block_len + offsets
        live.append(placed < length)
        distance.append((length - 1 - placed).astype(jnp.float32))

    def masks_of(g):
        low, high = spans[g]
        padded = -(-(high - low) // (16 * size)) * 16
        lane = lax.broadcasted_iota(jnp.int32, (padded, high - low), 1)
        row = lax.broadcasted_iota(jnp.int32, (padded, high - low), 0)
        head_row = lax.broadcasted_iota(jnp.int32, (padded, LANES), 0)
        head_lane = lax.broadcasted_iota(jnp.int32, (padded, LANES), 1)
        first, last = groups[g]
        slope = jnp.zeros((padded, LANES), jnp.float32)
        for h in range(first, last):
            slope = jnp.where(head_row == h - first, slopes[h], slope)
        return (lane >= row * size) & (lane < row * size + size), head_row == head_lane, slope[:, :1]

    masks = [masks_of(g) for g in range(len(groups))]

    def scores_of(g):
        low, high = spans[g]
        return [
            jnp.dot(
                jnp.where(masks[g][0], q_rows[b][:, low:high], 0.0).astype(jnp.bfloat16),
                kt_buf[b, low:high, :],
                preferred_element_type=jnp.float32,
            )
            for b in range(blocks)
        ]

    def values_of(g, scores):
        low, high = spans[g]
        of_head, diagonal, slope = masks[g]
        summed, inverse, stat_rows = [], [], []
        for b in range(blocks):
            score = jnp.where(live[b], scores[b] * scale - slope * distance[b], -1e30)
            top = jnp.max(score, axis=1, keepdims=True)
            weight_b = jnp.where(live[b], jnp.exp(score - top), 0.0)
            summed.append(
                jnp.dot(
                    weight_b.astype(jnp.bfloat16),
                    v_buf[b, :, low:high],
                    preferred_element_type=jnp.float32,
                )
            )
            total = jnp.sum(weight_b, axis=1, keepdims=True)
            inverse.append(1.0 / total)
            stat = jnp.sum(
                jnp.where(diagonal, top + jnp.log(total), 0.0), axis=0, keepdims=True
            )
            stat_rows.append(
                jnp.where(stat_lane == OWNER_LANE, owners[b].astype(jnp.float32), stat)
            )
        stats[g][me] = jnp.concatenate(stat_rows, axis=0)
        to_seq(stats[g], s_send.at[g], s_recv.at[g])
        acc_rows = [
            jnp.sum(jnp.where(of_head, summed[b] * inverse[b], 0.0), axis=0, keepdims=True)
            for b in range(blocks)
        ]
        accs[g][me] = jnp.concatenate(acc_rows, axis=0).astype(jnp.bfloat16)
        to_seq(accs[g], a_send.at[g], a_recv.at[g])

    scores = [scores_of(g) for g in range(min(2, len(groups)))]
    for g in range(len(groups)):
        values_of(g, scores[g])
        if g + 2 < len(groups):
            scores.append(scores_of(g + 2))

    def joined(ref):
        return jnp.concatenate([ref[j].astype(jnp.float32) for j in range(seq_size)], axis=0)

    def factors_of(g):
        stat = joined(stats[g])
        owner = stat[:, OWNER_LANE:]
        best, whole = jnp.zeros_like(stat), jnp.ones_like(stat)
        owned = [owner == float(s) for s in range(seqs)]
        for s in range(seqs):
            top = jnp.max(jnp.where(owned[s], stat, -1e30), axis=0, keepdims=True)
            best = jnp.where(owned[s], top, best)
        grown = jnp.exp(stat - best)
        for s in range(seqs):
            total = jnp.sum(jnp.where(owned[s], grown, 0.0), axis=0, keepdims=True)
            whole = jnp.where(owned[s], total, whole)
        factor = grown / whole
        first, last = groups[g]
        spread = jnp.concatenate(
            [jnp.broadcast_to(factor[:, h : h + 1], (factor.shape[0], size)) for h in range(last - first)],
            axis=1,
        )
        return spread, owner

    def attention_of(g):
        spread, owner = factors_of(g)
        scaled = joined(accs[g]) * spread
        seq_row = lax.broadcasted_iota(jnp.int32, (seqs, LANES), 0).astype(jnp.float32)
        if seqs <= 16:
            parts = []
            for low in range(0, scaled.shape[1], LANES):
                part_sum = jnp.zeros((seqs, LANES), jnp.float32)
                for i in range(scaled.shape[0]):
                    part_sum = part_sum + jnp.where(
                        owner[i : i + 1] == seq_row, scaled[i : i + 1, low : low + LANES], 0.0
                    )
                parts.append(part_sum)
            attention = jnp.concatenate(parts, axis=1)
        else:
            seq_lane = lax.broadcasted_iota(jnp.int32, (scaled.shape[0], LANES), 1)
            owned = jnp.where(owner == seq_lane.astype(jnp.float32), 1.0, 0.0)
            owned = owned.T[:seqs].astype(jnp.bfloat16)
            upper = scaled.astype(jnp.bfloat16)
            lower = (scaled - upper.astype(jnp.float32)).astype(jnp.bfloat16)
            attention = jnp.dot(owned, upper, preferred_element_type=jnp.float32) + jnp.dot(
                owned, lower, preferred_element_type=jnp.float32
            )
        return attention.astype(jnp.bfloat16)

    def project(g, attention, left, right):
        if left == right:
            return
        low, high = spans[g]
        product = jnp.dot(
            attention, w_buf[low:high, left:right], preferred_element_type=jnp.float32
        )
        held[:, left:right] = product if g == 0 else held[:, left:right] + product

    half = chunks // 2 * width
    columns_of = held.shape[1]
    attention = None
    for g, (low, high) in enumerate(spans):
        drain(stats[g].at[others], s_recv.at[g])
        drain(accs[g].at[others], a_recv.at[g])
        w_copies[g].wait()
        if g > 0:
            project(g - 1, attention, half, columns_of)
        attention = attention_of(g)
        if g + 1 < len(groups):
            project(g, attention, 0, half)

    def product_of(c):
        columns = slice(c * width, (c + 1) * width)
        product = jnp.dot(attention, w_buf[low:high, columns], preferred_element_type=jnp.float32)
        return product + held[:, columns]

    later = product_of(0)
    for c in range(chunks):
        product = later
        if c + 1 < chunks:
            later = product_of(c + 1)
        for r in range(tensor_size):
            part[r, c] = product[r * rows : (r + 1) * rows].astype(part.dtype)
        for k in range(1, tensor_size):
            peer = lax.rem(my_rows + k, tensor_size)
            pltpu.make_async_remote_copy(
                src_ref=part.at[peer, c],
                dst_ref=landed.at[k - 1, c],
                send_sem=p_send,
                recv_sem=p_recv,
                device_id={"tensor": peer},
            ).start()
    drain(landed, p_recv)
    for c in range(chunks):
        total = part[my_rows, c].astype(jnp.float32)
        for k in range(1, tensor_size):
            total = total + landed[k - 1, c].astype(jnp.float32)
        out[:, c * width : (c + 1) * width] = total.astype(out.dtype)
    for sent, copy in q_copies:
        pl.when(sent)(copy.wait_send)
    if paired:

        @pl.when(relay)
        def _():
            drain(q_pair.at[others], pair_send)

        @pl.when(jnp.logical_not(relay) & (me < seq_size - 1))
        def _():
            drain(q_pair.at[0], pair_send)

    for g in range(len(groups)):
        drain(stats[g].at[others], s_send.at[g])
        drain(accs[g].at[others], a_send.at[g])
    drain(landed, p_send)


def local(seq_size, tensor_size, query, key_cache, value_cache, slopes, block_seq, block_pos, lengths, weight):
    heads = slopes.shape[0]
    blocks, block_len, features = key_cache.shape
    size = features // heads
    columns = weight.shape[1]
    chunks = max([c for c in range(1, 9) if columns % (c * 256) == 0], default=1)
    width = columns // chunks
    rows = lengths.shape[0] // tensor_size
    outer = min(heads, -(-heads // 8) * 2)
    bounds = (0, outer, max(outer, heads - outer), heads)
    groups = [(low, high) for low, high in zip(bounds, bounds[1:]) if high > low]
    smalls = (block_seq, block_pos, lengths, slopes)
    dma = pltpu.SemaphoreType.DMA
    return pl.pallas_call(
        functools.partial(kernel, seq_size, tensor_size, groups, chunks),
        out_shape=pltpu.VMEM((rows, columns), jnp.bfloat16),
        in_specs=[pl.BlockSpec(memory_space=pltpu.HBM)] * 8,
        out_specs=pl.BlockSpec(memory_space=pltpu.VMEM),
        scratch_shapes=[pltpu.SMEM(a.shape, a.dtype) for a in smalls]
        + [
            pltpu.VMEM((seq_size,) + query.shape, query.dtype),
            pltpu.VMEM((seq_size,) + query.shape, query.dtype),
            pltpu.VMEM(key_cache.shape, key_cache.dtype),
            pltpu.VMEM((blocks, features, block_len), key_cache.dtype),
            pltpu.VMEM(value_cache.shape, value_cache.dtype),
            pltpu.VMEM(weight.shape, weight.dtype),
            [pltpu.VMEM((seq_size, blocks, LANES), jnp.float32) for _ in groups],
            [
                pltpu.VMEM((seq_size, blocks, (high - low) * size), jnp.bfloat16)
                for low, high in groups
            ],
            pltpu.VMEM((lengths.shape[0], columns), jnp.float32),
            pltpu.VMEM((tensor_size, chunks, rows, width), jnp.bfloat16),
            pltpu.VMEM((tensor_size - 1, chunks, rows, width), jnp.bfloat16),
            dma((4,)),
            dma,
            dma((blocks,)),
            dma,
            dma((len(groups),)),
        ]
        + [dma((seq_size - 1,)), dma, dma, dma((seq_size,))]
        + [dma((len(groups),))] * 4
        + [dma] * 2,
        compiler_params=pltpu.CompilerParams(
            collective_id=0, has_side_effects=True, vmem_limit_bytes=48 * 1024 * 1024
        ),
    )(
        *[
            pltpu.with_memory_space_constraint(a, pltpu.HBM)
            for a in smalls + (query, key_cache, value_cache, weight)
        ]
    )


def solution(mesh):
    placed = (
        P(("group", "seq"), "tensor"),
        P(("group", "seq"), None, "tensor"),
        P(("group", "seq"), None, "tensor"),
        P("tensor"),
        P(("group", "seq")),
        P(("group", "seq")),
        P("group"),
        P("tensor", "seq"),
    )
    return jax.shard_map(
        functools.partial(local, mesh.shape["seq"], mesh.shape["tensor"]),
        mesh=mesh,
        in_specs=placed,
        out_specs=P(("group", "tensor"), "seq"),
        check_vma=False,
    )
```

```python
import functools
import math

import jax
import jax.numpy as jnp
from jax import lax
from jax.experimental import pallas as pl
from jax.experimental.pallas import tpu as pltpu
from jax.sharding import PartitionSpec as P

LANES = 128
OWNER_LANE = LANES - 1


def kernel(
    seq_size, tensor_size, groups, chunks,
    block_seq_in, block_pos_in, lengths_in, slopes_in, query, keys, values, weight,
    out,
    block_seq, block_pos, lengths, slopes,
    q_all, q_pair, k_buf, kt_buf, v_buf, w_buf, stats, accs, held, part, landed,
    small_sem, q_sem, k_sem, v_sem, w_sem,
    q_send, q_recv, pair_send, pair_recv, ready, s_send, s_recv, a_send, a_recv, p_send, p_recv,
):
    me = lax.axis_index("seq")
    my_rows = lax.axis_index("tensor")
    blocks, block_len, features = k_buf.shape
    heads = slopes.shape[0]
    size = features // heads
    seqs = lengths.shape[0]
    query_rows = q_all.shape[1]
    rows, width = part.shape[2:]
    scale = 1.0 / math.sqrt(size)

    barrier = pltpu.get_barrier_semaphore()
    paired = tensor_size % 2 == 0
    plain = lax.rem(my_rows, 2) == 0
    partner = my_rows + 1 - 2 * lax.rem(my_rows, 2)
    steps = range(1, seq_size)

    def signal(when, **where):
        @pl.when(when)
        def _():
            pl.semaphore_signal(barrier, inc=1, device_id=where)

    for k in steps[::-1] if paired else ():
        lower = lax.rem(me + seq_size - k, seq_size)
        signal(plain & (me - k >= 1), seq=lower, tensor=partner)
    for k in steps:
        odd = jnp.logical_not(plain) if paired else me >= 0
        signal(odd | (me + k < seq_size), seq=lax.rem(me + k, seq_size))
    if paired:
        signal(jnp.logical_not(plain) & (me >= 1), seq=lax.rem(me + seq_size - 1, seq_size), tensor=partner)
    upper = [my_rows + k < tensor_size for k in range(1, tensor_size)]
    peers = [lax.rem(my_rows + k, tensor_size) for k in range(1, tensor_size)]
    for above, peer in zip(upper, peers):
        signal(above, tensor=peer)

    q_copy = pltpu.make_async_copy(query, q_all.at[me], q_sem)
    q_copy.start()
    small_copies = [
        pltpu.make_async_copy(source, target, small_sem.at[i])
        for i, (source, target) in enumerate(
            [
                (block_seq_in, block_seq),
                (block_pos_in, block_pos),
                (lengths_in, lengths),
                (slopes_in, slopes),
            ]
        )
    ]
    for copy in small_copies:
        copy.start()
    cache_copies = [
        pltpu.make_async_copy(keys.at[b], k_buf.at[b], k_sem.at[b]) for b in range(blocks)
    ] + [pltpu.make_async_copy(values.at[b], v_buf.at[b], v_sem) for b in range(blocks)]
    spans = [(first * size, last * size) for first, last in groups]
    w_copies = [
        pltpu.make_async_copy(
            weight.at[pl.ds(low, high - low)], w_buf.at[pl.ds(low, high - low)], w_sem.at[g]
        )
        for g, (low, high) in enumerate(spans)
    ]

    q_copy.wait()
    for copy in cache_copies:
        copy.start()
    last = seq_size - 1
    greeted = last
    if paired:
        from_plain = me + jnp.where(me < last, 1, 0)
        greeted = jnp.where(plain, from_plain, last + jnp.where(me >= 1, last - me, 0))
    if seq_size > 1:
        pl.semaphore_wait(barrier, greeted + my_rows)
    else:

        @pl.when(my_rows > 0)
        def _():
            pl.semaphore_wait(barrier, my_rows)

    for above, peer in zip(upper, peers):

        @pl.when(jnp.logical_not(above))
        def _():
            pl.semaphore_signal(ready, inc=1, device_id={"tensor": peer})

    stride = jnp.where(me < seq_size // 2, seq_size - 1, 1)

    def drain(ref, sem):
        pltpu.make_async_copy(ref, ref, sem).wait()

    def to_seq(buffer, send, recv):
        copies = [
            pltpu.make_async_remote_copy(
                src_ref=buffer.at[me],
                dst_ref=buffer.at[me],
                send_sem=send,
                recv_sem=recv,
                device_id={"seq": lax.rem(me + stride * k, seq_size)},
            )
            for k in range(1, seq_size)
        ]
        for copy in copies:
            copy.start()

    def q_copy_to(source, target, send, recv, where):
        return pltpu.make_async_remote_copy(
            src_ref=source, dst_ref=target, send_sem=send, recv_sem=recv, device_id=where
        )

    others = pl.ds(0, last)
    q_copies = []

    def send(when, copy):
        q_copies.append((when, copy))
        pl.when(when)(copy.start)

    if paired and last:
        following = {"seq": lax.rem(me + 1, seq_size), "tensor": partner}
        send(plain & (me < last), q_copy_to(q_all.at[me], q_pair, pair_send.at[0], pair_recv, following))
    for k in steps:
        peer = lax.rem(me + stride * k, seq_size)
        to_peer = jnp.logical_not(plain) | (peer < me) if paired else me >= 0
        send(to_peer, q_copy_to(q_all.at[me], q_all.at[me], q_send.at[k - 1], q_recv, {"seq": peer}))
    for copy in w_copies:
        copy.start()
    if paired and last:
        relay = jnp.logical_not(plain) & (me >= 1)
        source = lax.rem(me + last, seq_size)

        @pl.when(relay)
        def _():
            drain(q_pair, pair_recv)

        for k in range(last - 1, -1, -1):
            target = {"seq": lax.rem(me + k, seq_size), "tensor": partner}
            send(
                relay & (me + k < seq_size),
                q_copy_to(q_pair, q_all.at[source], pair_send.at[k], q_recv, target),
            )

    for copy in small_copies:
        copy.wait()
    offsets = lax.broadcasted_iota(jnp.int32, (1, block_len), 1)
    stat_lane = lax.broadcasted_iota(jnp.int32, (1, LANES), 1)

    for b in range(blocks):
        cache_copies[b].wait()
        for low in range(0, features, size):
            kt_buf[b, low : low + size, :] = k_buf[b, :, low : low + size].T
    drain(v_buf, v_sem)
    drain(q_all.at[others], q_recv)
    owners = [block_seq[b] for b in range(blocks)]
    q_rows, live, distance = [], [], []
    for b in range(blocks):
        near = q_all[lax.div(owners[b], query_rows)].astype(jnp.float32)
        which = lax.rem(owners[b], query_rows)
        q_row = near[:1]
        for r in range(1, query_rows):
            q_row = jnp.where(which == r, near[r : r + 1], q_row)
        q_rows.append(q_row)
        length = lengths[owners[b]]
        placed = block_pos[b] * block_len + offsets
        live.append(placed < length)
        distance.append((length - 1 - placed).astype(jnp.float32))

    def masks_of(g):
        low, high = spans[g]
        padded = -(-(high - low) // (16 * size)) * 16
        lane = lax.broadcasted_iota(jnp.int32, (padded, high - low), 1)
        row = lax.broadcasted_iota(jnp.int32, (padded, high - low), 0)
        head_row = lax.broadcasted_iota(jnp.int32, (padded, LANES), 0)
        head_lane = lax.broadcasted_iota(jnp.int32, (padded, LANES), 1)
        first, last = groups[g]
        slope = jnp.zeros((padded, LANES), jnp.float32)
        for h in range(first, last):
            slope = jnp.where(head_row == h - first, slopes[h], slope)
        return (lane >= row * size) & (lane < row * size + size), head_row == head_lane, slope[:, :1]

    masks = [masks_of(g) for g in range(len(groups))]

    def scores_of(g):
        low, high = spans[g]
        return [
            jnp.dot(
                jnp.where(masks[g][0], q_rows[b][:, low:high], 0.0).astype(jnp.bfloat16),
                kt_buf[b, low:high, :],
                preferred_element_type=jnp.float32,
            )
            for b in range(blocks)
        ]

    def values_of(g, scores):
        low, high = spans[g]
        of_head, diagonal, slope = masks[g]
        summed, inverse, stat_rows = [], [], []
        for b in range(blocks):
            score = jnp.where(live[b], scores[b] * scale - slope * distance[b], -1e30)
            top = jnp.max(score, axis=1, keepdims=True)
            weight_b = jnp.where(live[b], jnp.exp(score - top), 0.0)
            summed.append(
                jnp.dot(
                    weight_b.astype(jnp.bfloat16),
                    v_buf[b, :, low:high],
                    preferred_element_type=jnp.float32,
                )
            )
            total = jnp.sum(weight_b, axis=1, keepdims=True)
            inverse.append(1.0 / total)
            stat = jnp.sum(
                jnp.where(diagonal, top + jnp.log(total), 0.0), axis=0, keepdims=True
            )
            stat_rows.append(
                jnp.where(stat_lane == OWNER_LANE, owners[b].astype(jnp.float32), stat)
            )
        stats[g][me] = jnp.concatenate(stat_rows, axis=0)
        to_seq(stats[g], s_send.at[g], s_recv.at[g])
        acc_rows = [
            jnp.sum(jnp.where(of_head, summed[b] * inverse[b], 0.0), axis=0, keepdims=True)
            for b in range(blocks)
        ]
        accs[g][me] = jnp.concatenate(acc_rows, axis=0).astype(jnp.bfloat16)
        to_seq(accs[g], a_send.at[g], a_recv.at[g])

    scores = [scores_of(g) for g in range(min(2, len(groups)))]
    for g in range(len(groups)):
        values_of(g, scores[g])
        if g + 2 < len(groups):
            scores.append(scores_of(g + 2))

    def joined(ref):
        return jnp.concatenate([ref[j].astype(jnp.float32) for j in range(seq_size)], axis=0)

    def factors_of(g):
        stat = joined(stats[g])
        owner = stat[:, OWNER_LANE:]
        best, whole = jnp.zeros_like(stat), jnp.ones_like(stat)
        owned = [owner == float(s) for s in range(seqs)]
        for s in range(seqs):
            top = jnp.max(jnp.where(owned[s], stat, -1e30), axis=0, keepdims=True)
            best = jnp.where(owned[s], top, best)
        grown = jnp.exp(stat - best)
        for s in range(seqs):
            total = jnp.sum(jnp.where(owned[s], grown, 0.0), axis=0, keepdims=True)
            whole = jnp.where(owned[s], total, whole)
        factor = grown / whole
        first, last = groups[g]
        spread = jnp.concatenate(
            [jnp.broadcast_to(factor[:, h : h + 1], (factor.shape[0], size)) for h in range(last - first)],
            axis=1,
        )
        return spread, owner

    def attention_of(g, spread, owner):
        scaled = joined(accs[g]) * spread
        seq_row = lax.broadcasted_iota(jnp.int32, (seqs, LANES), 0).astype(jnp.float32)
        if seqs <= 16:
            parts = []
            for low in range(0, scaled.shape[1], LANES):
                part_sum = jnp.zeros((seqs, LANES), jnp.float32)
                for i in range(scaled.shape[0]):
                    part_sum = part_sum + jnp.where(
                        owner[i : i + 1] == seq_row, scaled[i : i + 1, low : low + LANES], 0.0
                    )
                parts.append(part_sum)
            attention = jnp.concatenate(parts, axis=1)
        else:
            seq_lane = lax.broadcasted_iota(jnp.int32, (scaled.shape[0], LANES), 1)
            owned = jnp.where(owner == seq_lane.astype(jnp.float32), 1.0, 0.0)
            owned = owned.T[:seqs].astype(jnp.bfloat16)
            upper = scaled.astype(jnp.bfloat16)
            lower = (scaled - upper.astype(jnp.float32)).astype(jnp.bfloat16)
            attention = jnp.dot(owned, upper, preferred_element_type=jnp.float32) + jnp.dot(
                owned, lower, preferred_element_type=jnp.float32
            )
        return attention.astype(jnp.bfloat16)

    @pl.when(my_rows < tensor_size - 1)
    def _():
        pl.semaphore_wait(ready, tensor_size - 1 - my_rows)

    def project(g, attention, left, right):
        if left == right:
            return
        low, high = spans[g]
        product = jnp.dot(
            attention, w_buf[low:high, left:right], preferred_element_type=jnp.float32
        )
        held[:, left:right] = product if g == 0 else held[:, left:right] + product

    half = chunks // 2 * width
    columns_of = held.shape[1]
    attention = None
    for g, (low, high) in enumerate(spans):
        w_copies[g].wait()
        drain(stats[g].at[others], s_recv.at[g])
        if g == 0:
            factors = factors_of(g)
        drain(accs[g].at[others], a_recv.at[g])
        if g > 0:
            factors = factors_of(g)
            project(g - 1, attention, half, columns_of)
        attention = attention_of(g, *factors)
        if g + 1 < len(groups):
            project(g, attention, 0, half)

    def product_of(c):
        columns = slice(c * width, (c + 1) * width)
        product = jnp.dot(attention, w_buf[low:high, columns], preferred_element_type=jnp.float32)
        return product + held[:, columns]

    later = product_of(0)
    for c in range(chunks):
        product = later
        if c + 1 < chunks:
            later = product_of(c + 1)
        for r in range(tensor_size):
            part[r, c] = product[r * rows : (r + 1) * rows].astype(part.dtype)
        for k in range(1, tensor_size):
            peer = lax.rem(my_rows + k, tensor_size)
            pltpu.make_async_remote_copy(
                src_ref=part.at[peer, c],
                dst_ref=landed.at[k - 1, c],
                send_sem=p_send,
                recv_sem=p_recv,
                device_id={"tensor": peer},
            ).start()
    drain(landed, p_recv)
    for c in range(chunks):
        total = part[my_rows, c].astype(jnp.float32)
        for k in range(1, tensor_size):
            total = total + landed[k - 1, c].astype(jnp.float32)
        out[:, c * width : (c + 1) * width] = total.astype(out.dtype)
    for sent, copy in q_copies:
        pl.when(sent)(copy.wait_send)
    for g in range(len(groups)):
        drain(stats[g].at[others], s_send.at[g])
        drain(accs[g].at[others], a_send.at[g])
    drain(landed, p_send)


def local(seq_size, tensor_size, query, key_cache, value_cache, slopes, block_seq, block_pos, lengths, weight):
    heads = slopes.shape[0]
    blocks, block_len, features = key_cache.shape
    size = features // heads
    columns = weight.shape[1]
    chunks = max([c for c in range(1, 9) if columns % (c * 256) == 0], default=1)
    width = columns // chunks
    rows = lengths.shape[0] // tensor_size
    bounds = [0, max(1, heads * 3 // 7), heads]
    groups = [(low, high) for low, high in zip(bounds, bounds[1:]) if high > low]
    smalls = (block_seq, block_pos, lengths, slopes)
    dma = pltpu.SemaphoreType.DMA
    return pl.pallas_call(
        functools.partial(kernel, seq_size, tensor_size, groups, chunks),
        out_shape=pltpu.VMEM((rows, columns), jnp.bfloat16),
        in_specs=[pl.BlockSpec(memory_space=pltpu.HBM)] * 8,
        out_specs=pl.BlockSpec(memory_space=pltpu.VMEM),
        scratch_shapes=[pltpu.SMEM(a.shape, a.dtype) for a in smalls]
        + [
            pltpu.VMEM((seq_size,) + query.shape, query.dtype),
            pltpu.VMEM(query.shape, query.dtype),
            pltpu.VMEM(key_cache.shape, key_cache.dtype),
            pltpu.VMEM((blocks, features, block_len), key_cache.dtype),
            pltpu.VMEM(value_cache.shape, value_cache.dtype),
            pltpu.VMEM(weight.shape, weight.dtype),
            [pltpu.VMEM((seq_size, blocks, LANES), jnp.float32) for _ in groups],
            [
                pltpu.VMEM((seq_size, blocks, (high - low) * size), jnp.bfloat16)
                for low, high in groups
            ],
            pltpu.VMEM((lengths.shape[0], columns), jnp.float32),
            pltpu.VMEM((tensor_size, chunks, rows, width), jnp.bfloat16),
            pltpu.VMEM((tensor_size - 1, chunks, rows, width), jnp.bfloat16),
            dma((4,)),
            dma,
            dma((blocks,)),
            dma,
            dma((len(groups),)),
        ]
        + [dma((max(1, seq_size - 1),)), dma, dma((max(1, seq_size - 1),)), dma, pltpu.SemaphoreType.REGULAR]
        + [dma((len(groups),))] * 4
        + [dma] * 2,
        compiler_params=pltpu.CompilerParams(
            collective_id=0, has_side_effects=True, vmem_limit_bytes=48 * 1024 * 1024
        ),
    )(
        *[
            pltpu.with_memory_space_constraint(a, pltpu.HBM)
            for a in smalls + (query, key_cache, value_cache, weight)
        ]
    )


def solution(mesh):
    placed = (
        P(("group", "seq"), "tensor"),
        P(("group", "seq"), None, "tensor"),
        P(("group", "seq"), None, "tensor"),
        P("tensor"),
        P(("group", "seq")),
        P(("group", "seq")),
        P("group"),
        P("tensor", "seq"),
    )
    return jax.shard_map(
        functools.partial(local, mesh.shape["seq"], mesh.shape["tensor"]),
        mesh=mesh,
        in_specs=placed,
        out_specs=P(("group", "tensor"), "seq"),
        check_vma=False,
    )
```

```python
import functools
import math

import jax
import jax.numpy as jnp
from jax import lax
from jax.experimental import pallas as pl
from jax.experimental.pallas import tpu as pltpu
from jax.sharding import PartitionSpec as P

LANES = 128
OWNER_LANE = LANES - 1


def kernel(
    seq_size, tensor_size, groups, chunks,
    block_seq_in, block_pos_in, lengths_in, slopes_in, query, keys, values, weight,
    out,
    block_seq, block_pos, lengths, slopes,
    q_all, q_pair, k_buf, kt_buf, v_buf, w_buf, accs, held, part, landed,
    small_sem, q_sem, k_sem, v_sem, w_sem,
    q_send, q_recv, pair_send, pair_recv, ready, a_send, a_recv, p_send, p_recv,
):
    me = lax.axis_index("seq")
    my_rows = lax.axis_index("tensor")
    blocks, block_len, features = k_buf.shape
    heads = slopes.shape[0]
    size = features // heads
    seqs = lengths.shape[0]
    query_rows = q_all.shape[1]
    rows = part.shape[1]
    scale = 1.0 / math.sqrt(size)

    q_copy = pltpu.make_async_copy(query, q_all.at[me], q_sem)
    q_copy.start()
    barrier = pltpu.get_barrier_semaphore()
    paired = tensor_size % 2 == 0
    plain = lax.rem(my_rows, 2) == 0
    partner = my_rows + 1 - 2 * lax.rem(my_rows, 2)
    steps = range(1, seq_size)

    def signal(when, **where):
        @pl.when(when)
        def _():
            pl.semaphore_signal(barrier, inc=1, device_id=where)

    for k in steps[::-1] if paired else ():
        lower = lax.rem(me + seq_size - k, seq_size)
        signal(plain & (me - k >= 1), seq=lower, tensor=partner)
    for k in steps:
        odd = jnp.logical_not(plain) if paired else me >= 0
        signal(odd | (me + k < seq_size), seq=lax.rem(me + k, seq_size))
    if paired:
        signal(jnp.logical_not(plain) & (me >= 1), seq=lax.rem(me + seq_size - 1, seq_size), tensor=partner)
    upper = [my_rows + k < tensor_size for k in range(1, tensor_size)]
    peers = [lax.rem(my_rows + k, tensor_size) for k in range(1, tensor_size)]
    for above, peer in zip(upper, peers):
        signal(above, tensor=peer)

    small_copies = [
        pltpu.make_async_copy(source, target, small_sem.at[i])
        for i, (source, target) in enumerate(
            [
                (block_seq_in, block_seq),
                (block_pos_in, block_pos),
                (lengths_in, lengths),
                (slopes_in, slopes),
            ]
        )
    ]
    for copy in small_copies:
        copy.start()
    cache_copies = [
        pltpu.make_async_copy(keys.at[b], k_buf.at[b], k_sem.at[b]) for b in range(blocks)
    ] + [pltpu.make_async_copy(values.at[b], v_buf.at[b], v_sem) for b in range(blocks)]
    spans = [(first * size, last * size) for first, last in groups]
    places = []
    for low, high in spans:
        start = places[-1].stop if places else 0
        places.append(slice(start, start + high - low + 3 * LANES))
    w_copies = [
        pltpu.make_async_copy(
            weight.at[pl.ds(low, high - low)], w_buf.at[pl.ds(low, high - low)], w_sem
        )
        for low, high in spans
    ]

    q_copy.wait()
    for copy in cache_copies:
        copy.start()
    last = seq_size - 1
    greeted = last
    if paired:
        from_plain = me + jnp.where(me < last, 1, 0)
        greeted = jnp.where(plain, from_plain, last + jnp.where(me >= 1, last - me, 0))
    if seq_size > 1:
        pl.semaphore_wait(barrier, greeted + my_rows)
    else:

        @pl.when(my_rows > 0)
        def _():
            pl.semaphore_wait(barrier, my_rows)

    for above, peer in zip(upper, peers):

        @pl.when(jnp.logical_not(above))
        def _():
            pl.semaphore_signal(ready, inc=1, device_id={"tensor": peer})

    stride = jnp.where(me < seq_size // 2, seq_size - 1, 1)

    def drain(ref, sem):
        pltpu.make_async_copy(ref, ref, sem).wait()

    def to_seq(buffer, where, send, recv):
        copies = [
            pltpu.make_async_remote_copy(
                src_ref=buffer.at[me, :, where],
                dst_ref=buffer.at[me, :, where],
                send_sem=send,
                recv_sem=recv,
                device_id={"seq": lax.rem(me + stride * k, seq_size)},
            )
            for k in range(1, seq_size)
        ]
        for copy in copies:
            copy.start()

    def q_copy_to(source, target, send, recv, where):
        return pltpu.make_async_remote_copy(
            src_ref=source, dst_ref=target, send_sem=send, recv_sem=recv, device_id=where
        )

    others = pl.ds(0, last)
    q_copies = []

    def send(when, copy):
        q_copies.append((when, copy))
        pl.when(when)(copy.start)

    if paired and last:
        following = {"seq": lax.rem(me + 1, seq_size), "tensor": partner}
        send(plain & (me < last), q_copy_to(q_all.at[me], q_pair, pair_send.at[0], pair_recv, following))
    for k in steps:
        peer = lax.rem(me + stride * k, seq_size)
        to_peer = jnp.logical_not(plain) | (peer < me) if paired else me >= 0
        send(to_peer, q_copy_to(q_all.at[me], q_all.at[me], q_send.at[k - 1], q_recv, {"seq": peer}))
    for copy in w_copies:
        copy.start()
    if paired and last:
        relay = jnp.logical_not(plain) & (me >= 1)
        source = lax.rem(me + last, seq_size)

        @pl.when(relay)
        def _():
            drain(q_pair, pair_recv)

        for k in range(last - 1, -1, -1):
            target = {"seq": lax.rem(me + k, seq_size), "tensor": partner}
            send(
                relay & (me + k < seq_size),
                q_copy_to(q_pair, q_all.at[source], pair_send.at[k], q_recv, target),
            )

    for copy in small_copies:
        copy.wait()
    offsets = lax.broadcasted_iota(jnp.int32, (1, block_len), 1)
    stat_lane = lax.broadcasted_iota(jnp.int32, (1, LANES), 1)

    for b in range(blocks):
        cache_copies[b].wait()
        for low in range(0, features, size):
            kt_buf[b, low : low + size, :] = k_buf[b, :, low : low + size].T
    drain(v_buf, v_sem)
    drain(q_all.at[others], q_recv)
    owners = [block_seq[b] for b in range(blocks)]
    q_rows, live, distance = [], [], []
    for b in range(blocks):
        near = q_all[lax.div(owners[b], query_rows)].astype(jnp.float32)
        which = lax.rem(owners[b], query_rows)
        q_row = near[:1]
        for r in range(1, query_rows):
            q_row = jnp.where(which == r, near[r : r + 1], q_row)
        q_rows.append(q_row)
        length = lengths[owners[b]]
        placed = block_pos[b] * block_len + offsets
        live.append(placed < length)
        distance.append((length - 1 - placed).astype(jnp.float32))

    def masks_of(g):
        low, high = spans[g]
        padded = -(-(high - low) // (16 * size)) * 16
        lane = lax.broadcasted_iota(jnp.int32, (padded, high - low), 1)
        row = lax.broadcasted_iota(jnp.int32, (padded, high - low), 0)
        head_row = lax.broadcasted_iota(jnp.int32, (padded, LANES), 0)
        head_lane = lax.broadcasted_iota(jnp.int32, (padded, LANES), 1)
        first, last = groups[g]
        slope = jnp.zeros((padded, LANES), jnp.float32)
        for h in range(first, last):
            slope = jnp.where(head_row == h - first, slopes[h], slope)
        return (lane >= row * size) & (lane < row * size + size), head_row == head_lane, slope[:, :1]

    masks = [masks_of(g) for g in range(len(groups))]

    def scores_of(g):
        low, high = spans[g]
        return [
            jnp.dot(
                jnp.where(masks[g][0], q_rows[b][:, low:high], 0.0).astype(jnp.bfloat16),
                kt_buf[b, low:high, :],
                preferred_element_type=jnp.float32,
            )
            for b in range(blocks)
        ]

    def values_of(g, scores):
        low, high = spans[g]
        of_head, diagonal, slope = masks[g]
        summed, inverse, stat_rows = [], [], []
        for b in range(blocks):
            score = jnp.where(live[b], scores[b] * scale - slope * distance[b], -1e30)
            top = jnp.max(score, axis=1, keepdims=True)
            weight_b = jnp.where(live[b], jnp.exp(score - top), 0.0)
            summed.append(
                jnp.dot(
                    weight_b.astype(jnp.bfloat16),
                    v_buf[b, :, low:high],
                    preferred_element_type=jnp.float32,
                )
            )
            total = jnp.sum(weight_b, axis=1, keepdims=True)
            inverse.append(1.0 / total)
            stat = jnp.sum(
                jnp.where(diagonal, top + jnp.log(total), 0.0), axis=0, keepdims=True
            )
            stat_rows.append(
                jnp.where(stat_lane == OWNER_LANE, owners[b].astype(jnp.float32), stat)
            )
        stat = jnp.concatenate(stat_rows, axis=0)
        pieces = []
        for _ in range(3):
            pieces.append(stat.astype(jnp.bfloat16))
            stat = stat - pieces[-1].astype(jnp.float32)
        acc_rows = [
            jnp.sum(jnp.where(of_head, summed[b] * inverse[b], 0.0), axis=0, keepdims=True)
            for b in range(blocks)
        ]
        acc = jnp.concatenate(acc_rows, axis=0).astype(jnp.bfloat16)
        where = places[g]
        accs[me, :, where] = jnp.concatenate([acc] + pieces, axis=1)
        to_seq(accs, where, a_send, a_recv.at[g])

    scores = [scores_of(g) for g in range(min(2, len(groups)))]
    for g in range(len(groups)):
        values_of(g, scores[g])
        if g + 2 < len(groups):
            scores.append(scores_of(g + 2))

    def joined(ref, low, high):
        return jnp.concatenate(
            [ref[j, :, low:high].astype(jnp.float32) for j in range(seq_size)], axis=0
        )

    def factors_of(g):
        low, high = spans[g]
        stat = jnp.zeros((), jnp.float32)
        for i in range(3):
            start = places[g].start + high - low + i * LANES
            stat = stat + joined(accs, start, start + LANES)
        owner = stat[:, OWNER_LANE:]
        best, whole = jnp.zeros_like(stat), jnp.ones_like(stat)
        owned = [owner == float(s) for s in range(seqs)]
        for s in range(seqs):
            top = jnp.max(jnp.where(owned[s], stat, -1e30), axis=0, keepdims=True)
            best = jnp.where(owned[s], top, best)
        grown = jnp.exp(stat - best)
        for s in range(seqs):
            total = jnp.sum(jnp.where(owned[s], grown, 0.0), axis=0, keepdims=True)
            whole = jnp.where(owned[s], total, whole)
        factor = grown / whole
        first, last = groups[g]
        spread = jnp.concatenate(
            [jnp.broadcast_to(factor[:, h : h + 1], (factor.shape[0], size)) for h in range(last - first)],
            axis=1,
        )
        return spread, owner

    def attention_of(g, spread, owner):
        start = places[g].start
        scaled = joined(accs, start, start + spread.shape[1]) * spread
        seq_row = lax.broadcasted_iota(jnp.int32, (seqs, LANES), 0).astype(jnp.float32)
        if seqs <= 16:
            parts = []
            for low in range(0, scaled.shape[1], LANES):
                part_sum = jnp.zeros((seqs, LANES), jnp.float32)
                for i in range(scaled.shape[0]):
                    part_sum = part_sum + jnp.where(
                        owner[i : i + 1] == seq_row, scaled[i : i + 1, low : low + LANES], 0.0
                    )
                parts.append(part_sum)
            attention = jnp.concatenate(parts, axis=1)
        else:
            seq_lane = lax.broadcasted_iota(jnp.int32, (scaled.shape[0], LANES), 1)
            owned = jnp.where(owner == seq_lane.astype(jnp.float32), 1.0, 0.0)
            owned = owned.T[:seqs].astype(jnp.bfloat16)
            upper = scaled.astype(jnp.bfloat16)
            lower = (scaled - upper.astype(jnp.float32)).astype(jnp.bfloat16)
            attention = jnp.dot(owned, upper, preferred_element_type=jnp.float32) + jnp.dot(
                owned, lower, preferred_element_type=jnp.float32
            )
        return attention.astype(jnp.bfloat16)

    @pl.when(my_rows < tensor_size - 1)
    def _():
        pl.semaphore_wait(ready, tensor_size - 1 - my_rows)

    def project(g, attention, left, right):
        if left == right:
            return
        low, high = spans[g]
        product = jnp.dot(
            attention, w_buf[low:high, left:right], preferred_element_type=jnp.float32
        )
        held[:, left:right] = product if g == 0 else held[:, left:right] + product

    half = held.shape[1] // (2 * LANES * 2) * (LANES * 2)
    columns_of = held.shape[1]
    attention = None
    for g, (low, high) in enumerate(spans):
        if g == 0:
            drain(w_buf, w_sem)
        drain(accs.at[others, :, places[g]], a_recv.at[g])
        factors = factors_of(g)
        if g > 0:
            project(g - 1, attention, half, columns_of)
        attention = attention_of(g, *factors)
        if g + 1 < len(groups):
            project(g, attention, 0, half)

    def product_of(columns):
        product = jnp.dot(attention, w_buf[low:high, columns], preferred_element_type=jnp.float32)
        return product + held[:, columns]

    later = product_of(chunks[0])
    for c, columns in enumerate(chunks):
        product = later
        if c + 1 < len(chunks):
            later = product_of(chunks[c + 1])
        for r in range(tensor_size):
            part[r, :, columns] = product[r * rows : (r + 1) * rows].astype(part.dtype)
        for k in range(1, tensor_size):
            peer = lax.rem(my_rows + k, tensor_size)
            pltpu.make_async_remote_copy(
                src_ref=part.at[peer, :, columns],
                dst_ref=landed.at[k - 1, :, columns],
                send_sem=p_send,
                recv_sem=p_recv,
                device_id={"tensor": peer},
            ).start()
    drain(landed, p_recv)
    total = part[my_rows].astype(jnp.float32)
    for k in range(1, tensor_size):
        total = total + landed[k - 1].astype(jnp.float32)
    out[...] = total.astype(out.dtype)
    for sent, copy in q_copies:
        pl.when(sent)(copy.wait_send)
    drain(accs.at[others], a_send)
    drain(landed, p_send)


def local(seq_size, tensor_size, query, key_cache, value_cache, slopes, block_seq, block_pos, lengths, weight):
    heads = slopes.shape[0]
    blocks, block_len, features = key_cache.shape
    size = features // heads
    columns = weight.shape[1]
    tiles = columns // (2 * LANES)
    cuts = [tiles * c // 4 * (2 * LANES) for c in range(4)] + [columns]
    chunks = [slice(low, high) for low, high in zip(cuts, cuts[1:]) if high > low]
    rows = lengths.shape[0] // tensor_size
    bounds = [0, heads * 2 // 7, heads * 4 // 7, heads]
    groups = [(low, high) for low, high in zip(bounds, bounds[1:]) if high > low]
    smalls = (block_seq, block_pos, lengths, slopes)
    dma = pltpu.SemaphoreType.DMA
    return pl.pallas_call(
        functools.partial(kernel, seq_size, tensor_size, groups, chunks),
        out_shape=pltpu.VMEM((rows, columns), jnp.bfloat16),
        in_specs=[pl.BlockSpec(memory_space=pltpu.HBM)] * 8,
        out_specs=pl.BlockSpec(memory_space=pltpu.VMEM),
        scratch_shapes=[pltpu.SMEM(a.shape, a.dtype) for a in smalls]
        + [
            pltpu.VMEM((seq_size,) + query.shape, query.dtype),
            pltpu.VMEM(query.shape, query.dtype),
            pltpu.VMEM(key_cache.shape, key_cache.dtype),
            pltpu.VMEM((blocks, features, block_len), key_cache.dtype),
            pltpu.VMEM(value_cache.shape, value_cache.dtype),
            pltpu.VMEM(weight.shape, weight.dtype),
            pltpu.VMEM((seq_size, blocks, features + 3 * LANES * len(groups)), jnp.bfloat16),
            pltpu.VMEM((lengths.shape[0], columns), jnp.float32),
            pltpu.VMEM((tensor_size, rows, columns), jnp.bfloat16),
            pltpu.VMEM((tensor_size - 1, rows, columns), jnp.bfloat16),
            dma((4,)),
            dma,
            dma((blocks,)),
            dma,
            dma,
        ]
        + [dma((max(1, seq_size - 1),)), dma, dma((max(1, seq_size - 1),)), dma, pltpu.SemaphoreType.REGULAR]
        + [dma, dma((len(groups),))]
        + [dma] * 2,
        compiler_params=pltpu.CompilerParams(
            collective_id=0, has_side_effects=True, vmem_limit_bytes=48 * 1024 * 1024
        ),
    )(
        *[
            pltpu.with_memory_space_constraint(a, pltpu.HBM)
            for a in smalls + (query, key_cache, value_cache, weight)
        ]
    )


def solution(mesh):
    placed = (
        P(("group", "seq"), "tensor"),
        P(("group", "seq"), None, "tensor"),
        P(("group", "seq"), None, "tensor"),
        P("tensor"),
        P(("group", "seq")),
        P(("group", "seq")),
        P("group"),
        P("tensor", "seq"),
    )
    return jax.shard_map(
        functools.partial(local, mesh.shape["seq"], mesh.shape["tensor"]),
        mesh=mesh,
        in_specs=placed,
        out_specs=P(("group", "tensor"), "seq"),
        check_vma=False,
    )
```

```python
import functools
import math

import jax
import jax.numpy as jnp
from jax import lax
from jax.experimental import pallas as pl
from jax.experimental.pallas import tpu as pltpu
from jax.sharding import PartitionSpec as P

LANES = 128


def kernel(
    seq_size, tensor_size, groups, chunks,
    block_seq_in, block_pos_in, lengths_in, slopes_in, query, keys, values, weight,
    out,
    block_seq, block_pos, lengths, slopes,
    q_all, q_pair, k_buf, kt_buf, v_buf, w_buf, accs, held, part, landed,
    small_sem, q_sem, k_sem, v_sem, w_sem,
    q_send, q_recv, pair_send, pair_recv, ready, a_send, a_recv, p_send, p_recv,
):
    me = lax.axis_index("seq")
    my_rows = lax.axis_index("tensor")
    blocks, block_len, features = k_buf.shape
    heads = slopes.shape[0]
    size = features // heads
    seqs = lengths.shape[0]
    query_rows = q_all.shape[1]
    rows = part.shape[1]
    scale = 1.0 / math.sqrt(size)

    q_copy = pltpu.make_async_copy(query, q_all.at[me], q_sem)
    q_copy.start()
    barrier = pltpu.get_barrier_semaphore()
    paired = tensor_size % 2 == 0
    plain = lax.rem(my_rows, 2) == 0
    partner = my_rows + 1 - 2 * lax.rem(my_rows, 2)
    steps = range(1, seq_size)

    def signal(when, **where):
        @pl.when(when)
        def _():
            pl.semaphore_signal(barrier, inc=1, device_id=where)

    for k in steps[::-1] if paired else ():
        lower = lax.rem(me + seq_size - k, seq_size)
        signal(plain & (me - k >= 1), seq=lower, tensor=partner)
    for k in steps:
        odd = jnp.logical_not(plain) if paired else me >= 0
        signal(odd | (me + k < seq_size), seq=lax.rem(me + k, seq_size))
    if paired:
        signal(jnp.logical_not(plain) & (me >= 1), seq=lax.rem(me + seq_size - 1, seq_size), tensor=partner)
    upper = [my_rows + k < tensor_size for k in range(1, tensor_size)]
    peers = [lax.rem(my_rows + k, tensor_size) for k in range(1, tensor_size)]
    for above, peer in zip(upper, peers):
        signal(above, tensor=peer)

    small_copies = [
        pltpu.make_async_copy(source, target, small_sem.at[i])
        for i, (source, target) in enumerate(
            [
                (block_seq_in, block_seq),
                (block_pos_in, block_pos),
                (lengths_in, lengths),
                (slopes_in, slopes),
            ]
        )
    ]
    for copy in small_copies:
        copy.start()
    cache_copies = [
        pltpu.make_async_copy(keys.at[b], k_buf.at[b], k_sem.at[b]) for b in range(blocks)
    ] + [pltpu.make_async_copy(values.at[b], v_buf.at[b], v_sem) for b in range(blocks)]
    spans = [(first * size, last * size) for first, last in groups]
    places = []
    for low, high in spans:
        start = places[-1].stop if places else 0
        places.append(slice(start, start + high - low + 4 * LANES))
    w_copies = [
        pltpu.make_async_copy(
            weight.at[pl.ds(low, high - low)], w_buf.at[pl.ds(low, high - low)], w_sem
        )
        for low, high in spans
    ]

    q_copy.wait()
    for copy in cache_copies:
        copy.start()
    last = seq_size - 1
    greeted = last
    if paired:
        from_plain = me + jnp.where(me < last, 1, 0)
        greeted = jnp.where(plain, from_plain, last + jnp.where(me >= 1, last - me, 0))
    if seq_size > 1:
        pl.semaphore_wait(barrier, greeted + my_rows)
    else:

        @pl.when(my_rows > 0)
        def _():
            pl.semaphore_wait(barrier, my_rows)

    for above, peer in zip(upper, peers):

        @pl.when(jnp.logical_not(above))
        def _():
            pl.semaphore_signal(ready, inc=1, device_id={"tensor": peer})

    stride = jnp.where(me < seq_size // 2, seq_size - 1, 1)

    def drain(ref, sem):
        pltpu.make_async_copy(ref, ref, sem).wait()

    def to_seq(buffer, where, send, recv):
        copies = [
            pltpu.make_async_remote_copy(
                src_ref=buffer.at[me, :, where],
                dst_ref=buffer.at[me, :, where],
                send_sem=send,
                recv_sem=recv,
                device_id={"seq": lax.rem(me + stride * k, seq_size)},
            )
            for k in range(1, seq_size)
        ]
        for copy in copies:
            copy.start()

    def q_copy_to(source, target, send, recv, where):
        return pltpu.make_async_remote_copy(
            src_ref=source, dst_ref=target, send_sem=send, recv_sem=recv, device_id=where
        )

    others = pl.ds(0, last)
    q_copies = []

    def send(when, copy):
        q_copies.append((when, copy))
        pl.when(when)(copy.start)

    if paired and last:
        following = {"seq": lax.rem(me + 1, seq_size), "tensor": partner}
        send(plain & (me < last), q_copy_to(q_all.at[me], q_pair, pair_send.at[0], pair_recv, following))
    for k in steps:
        peer = lax.rem(me + stride * k, seq_size)
        to_peer = jnp.logical_not(plain) | (peer < me) if paired else me >= 0
        send(to_peer, q_copy_to(q_all.at[me], q_all.at[me], q_send.at[k - 1], q_recv, {"seq": peer}))
    for copy in w_copies:
        copy.start()
    if paired and last:
        relay = jnp.logical_not(plain) & (me >= 1)
        source = lax.rem(me + last, seq_size)

        @pl.when(relay)
        def _():
            drain(q_pair, pair_recv)

        for k in range(last - 1, -1, -1):
            target = {"seq": lax.rem(me + k, seq_size), "tensor": partner}
            send(
                relay & (me + k < seq_size),
                q_copy_to(q_pair, q_all.at[source], pair_send.at[k], q_recv, target),
            )

    for copy in small_copies:
        copy.wait()
    offsets = lax.broadcasted_iota(jnp.int32, (1, block_len), 1)

    for b in range(blocks):
        cache_copies[b].wait()
        for low in range(0, features, size):
            kt_buf[b, low : low + size, :] = k_buf[b, :, low : low + size].T
    drain(v_buf, v_sem)
    drain(q_all.at[others], q_recv)
    owners = [block_seq[b] for b in range(blocks)]
    q_rows, live, distance = [], [], []
    for b in range(blocks):
        near = q_all[lax.div(owners[b], query_rows)].astype(jnp.float32)
        which = lax.rem(owners[b], query_rows)
        q_row = near[:1]
        for r in range(1, query_rows):
            q_row = jnp.where(which == r, near[r : r + 1], q_row)
        q_rows.append(q_row)
        length = lengths[owners[b]]
        placed = block_pos[b] * block_len + offsets
        live.append(placed < length)
        distance.append((length - 1 - placed).astype(jnp.float32))

    def masks_of(g):
        low, high = spans[g]
        padded = -(-(high - low) // (16 * size)) * 16
        lane = lax.broadcasted_iota(jnp.int32, (padded, high - low), 1)
        row = lax.broadcasted_iota(jnp.int32, (padded, high - low), 0)
        head_row = lax.broadcasted_iota(jnp.int32, (padded, LANES), 0)
        head_lane = lax.broadcasted_iota(jnp.int32, (padded, LANES), 1)
        first, last = groups[g]
        slope = jnp.zeros((padded, LANES), jnp.float32)
        for h in range(first, last):
            slope = jnp.where(head_row == h - first, slopes[h], slope)
        return (lane >= row * size) & (lane < row * size + size), head_row == head_lane, slope[:, :1]

    masks = [masks_of(g) for g in range(len(groups))]

    def scores_of(g):
        low, high = spans[g]
        return [
            jnp.dot(
                jnp.where(masks[g][0], q_rows[b][:, low:high], 0.0).astype(jnp.bfloat16),
                kt_buf[b, low:high, :],
                preferred_element_type=jnp.float32,
            )
            for b in range(blocks)
        ]

    def values_of(g, scores):
        low, high = spans[g]
        of_head, diagonal, slope = masks[g]
        summed, inverse, stat_rows = [], [], []
        for b in range(blocks):
            score = jnp.where(live[b], scores[b] * scale - slope * distance[b], -1e30)
            top = jnp.max(score, axis=1, keepdims=True)
            weight_b = jnp.where(live[b], jnp.exp(score - top), 0.0)
            summed.append(
                jnp.dot(
                    weight_b.astype(jnp.bfloat16),
                    v_buf[b, :, low:high],
                    preferred_element_type=jnp.float32,
                )
            )
            total = jnp.sum(weight_b, axis=1, keepdims=True)
            inverse.append(1.0 / total)
            stat = jnp.sum(
                jnp.where(diagonal, top + jnp.log(total), 0.0), axis=0, keepdims=True
            )
            stat_rows.append(stat)
        stat = jnp.concatenate(stat_rows, axis=0)
        pieces = []
        for _ in range(3):
            pieces.append(stat.astype(jnp.bfloat16))
            stat = stat - pieces[-1].astype(jnp.float32)
        owner_rows = [
            jnp.broadcast_to(owners[b].astype(jnp.float32), (1, LANES)) for b in range(blocks)
        ]
        pieces.append(jnp.concatenate(owner_rows, axis=0).astype(jnp.bfloat16))
        acc_rows = [
            jnp.sum(jnp.where(of_head, summed[b] * inverse[b], 0.0), axis=0, keepdims=True)
            for b in range(blocks)
        ]
        acc = jnp.concatenate(acc_rows, axis=0).astype(jnp.bfloat16)
        where = places[g]
        accs[me, :, where] = jnp.concatenate([acc] + pieces, axis=1)
        to_seq(accs, where, a_send, a_recv.at[g])

    scores = [scores_of(g) for g in range(min(2, len(groups)))]
    for g in range(len(groups)):
        values_of(g, scores[g])
        if g + 2 < len(groups):
            scores.append(scores_of(g + 2))

    def joined(ref, low, high):
        return jnp.concatenate(
            [ref[j, :, low:high].astype(jnp.float32) for j in range(seq_size)], axis=0
        )

    def factors_of(g):
        low, high = spans[g]
        stat = jnp.zeros((), jnp.float32)
        for i in range(3):
            start = places[g].start + high - low + i * LANES
            stat = stat + joined(accs, start, start + LANES)
        owner = joined(accs, start + LANES, start + 2 * LANES)
        best, whole = jnp.zeros_like(stat), jnp.ones_like(stat)
        owned = [owner == float(s) for s in range(seqs)]
        for s in range(seqs):
            top = jnp.max(jnp.where(owned[s], stat, -1e30), axis=0, keepdims=True)
            best = jnp.where(owned[s], top, best)
        grown = jnp.exp(stat - best)
        for s in range(seqs):
            total = jnp.sum(jnp.where(owned[s], grown, 0.0), axis=0, keepdims=True)
            whole = jnp.where(owned[s], total, whole)
        factor = grown / whole
        first, last = groups[g]
        spread = jnp.concatenate(
            [jnp.broadcast_to(factor[:, h : h + 1], (factor.shape[0], size)) for h in range(last - first)],
            axis=1,
        )
        return spread, owner

    def attention_of(g, spread, owner):
        start = places[g].start
        scaled = joined(accs, start, start + spread.shape[1]) * spread
        seq_row = lax.broadcasted_iota(jnp.int32, (seqs, LANES), 0).astype(jnp.float32)
        if seqs <= 16:
            parts = []
            for low in range(0, scaled.shape[1], LANES):
                part_sum = jnp.zeros((seqs, LANES), jnp.float32)
                for i in range(scaled.shape[0]):
                    part_sum = part_sum + jnp.where(
                        owner[i : i + 1] == seq_row, scaled[i : i + 1, low : low + LANES], 0.0
                    )
                parts.append(part_sum)
            attention = jnp.concatenate(parts, axis=1)
        else:
            seq_lane = lax.broadcasted_iota(jnp.int32, (scaled.shape[0], LANES), 1)
            owned = jnp.where(owner == seq_lane.astype(jnp.float32), 1.0, 0.0)
            owned = owned.T[:seqs].astype(jnp.bfloat16)
            upper = scaled.astype(jnp.bfloat16)
            lower = (scaled - upper.astype(jnp.float32)).astype(jnp.bfloat16)
            attention = jnp.dot(owned, upper, preferred_element_type=jnp.float32) + jnp.dot(
                owned, lower, preferred_element_type=jnp.float32
            )
        return attention.astype(jnp.bfloat16)

    @pl.when(my_rows < tensor_size - 1)
    def _():
        pl.semaphore_wait(ready, tensor_size - 1 - my_rows)

    def project(g, attention, left, right):
        if left == right:
            return
        low, high = spans[g]
        product = jnp.dot(
            attention, w_buf[low:high, left:right], preferred_element_type=jnp.float32
        )
        held[:, left:right] = product if g == 0 else held[:, left:right] + product

    half = held.shape[1] // (2 * LANES * 2) * (LANES * 2)
    columns_of = held.shape[1]
    attention = None
    for g, (low, high) in enumerate(spans):
        if g == 0:
            drain(w_buf, w_sem)
        drain(accs.at[others, :, places[g]], a_recv.at[g])
        factors = factors_of(g)
        if g > 0:
            project(g - 1, attention, half, columns_of)
        attention = attention_of(g, *factors)
        if g + 1 < len(groups):
            project(g, attention, 0, half)

    def product_of(columns):
        product = jnp.dot(attention, w_buf[low:high, columns], preferred_element_type=jnp.float32)
        return product + held[:, columns]

    later = product_of(chunks[0])
    for c, columns in enumerate(chunks):
        product = later
        if c + 1 < len(chunks):
            later = product_of(chunks[c + 1])
        for r in range(tensor_size):
            part[r, :, columns] = product[r * rows : (r + 1) * rows].astype(part.dtype)
        for k in range(1, tensor_size):
            peer = lax.rem(my_rows + k, tensor_size)
            pltpu.make_async_remote_copy(
                src_ref=part.at[peer, :, columns],
                dst_ref=landed.at[k - 1, :, columns],
                send_sem=p_send,
                recv_sem=p_recv,
                device_id={"tensor": peer},
            ).start()
    drain(landed, p_recv)
    total = part[my_rows].astype(jnp.float32)
    for k in range(1, tensor_size):
        total = total + landed[k - 1].astype(jnp.float32)
    out[...] = total.astype(out.dtype)
    for sent, copy in q_copies:
        pl.when(sent)(copy.wait_send)
    drain(accs.at[others], a_send)
    drain(landed, p_send)


def local(seq_size, tensor_size, query, key_cache, value_cache, slopes, block_seq, block_pos, lengths, weight):
    heads = slopes.shape[0]
    blocks, block_len, features = key_cache.shape
    size = features // heads
    columns = weight.shape[1]
    tiles = columns // (2 * LANES)
    cuts = [tiles * c // 4 * (2 * LANES) for c in range(4)] + [columns]
    chunks = [slice(low, high) for low, high in zip(cuts, cuts[1:]) if high > low]
    rows = lengths.shape[0] // tensor_size
    bounds = [0, heads * 2 // 7, heads * 4 // 7, heads]
    groups = [(low, high) for low, high in zip(bounds, bounds[1:]) if high > low]
    smalls = (block_seq, block_pos, lengths, slopes)
    dma = pltpu.SemaphoreType.DMA
    return pl.pallas_call(
        functools.partial(kernel, seq_size, tensor_size, groups, chunks),
        out_shape=pltpu.VMEM((rows, columns), jnp.bfloat16),
        in_specs=[pl.BlockSpec(memory_space=pltpu.HBM)] * 8,
        out_specs=pl.BlockSpec(memory_space=pltpu.VMEM),
        scratch_shapes=[pltpu.SMEM(a.shape, a.dtype) for a in smalls]
        + [
            pltpu.VMEM((seq_size,) + query.shape, query.dtype),
            pltpu.VMEM(query.shape, query.dtype),
            pltpu.VMEM(key_cache.shape, key_cache.dtype),
            pltpu.VMEM((blocks, features, block_len), key_cache.dtype),
            pltpu.VMEM(value_cache.shape, value_cache.dtype),
            pltpu.VMEM(weight.shape, weight.dtype),
            pltpu.VMEM((seq_size, blocks, features + 4 * LANES * len(groups)), jnp.bfloat16),
            pltpu.VMEM((lengths.shape[0], columns), jnp.float32),
            pltpu.VMEM((tensor_size, rows, columns), jnp.bfloat16),
            pltpu.VMEM((tensor_size - 1, rows, columns), jnp.bfloat16),
            dma((4,)),
            dma,
            dma((blocks,)),
            dma,
            dma,
        ]
        + [dma((max(1, seq_size - 1),)), dma, dma((max(1, seq_size - 1),)), dma, pltpu.SemaphoreType.REGULAR]
        + [dma, dma((len(groups),))]
        + [dma] * 2,
        compiler_params=pltpu.CompilerParams(
            collective_id=0, has_side_effects=True, vmem_limit_bytes=48 * 1024 * 1024
        ),
    )(
        *[
            pltpu.with_memory_space_constraint(a, pltpu.HBM)
            for a in smalls + (query, key_cache, value_cache, weight)
        ]
    )


def solution(mesh):
    placed = (
        P(("group", "seq"), "tensor"),
        P(("group", "seq"), None, "tensor"),
        P(("group", "seq"), None, "tensor"),
        P("tensor"),
        P(("group", "seq")),
        P(("group", "seq")),
        P("group"),
        P("tensor", "seq"),
    )
    return jax.shard_map(
        functools.partial(local, mesh.shape["seq"], mesh.shape["tensor"]),
        mesh=mesh,
        in_specs=placed,
        out_specs=P(("group", "tensor"), "seq"),
        check_vma=False,
    )
```
